512 devices in a mesh: dp: 8 (over z_hi, core), mp: 64 (over z_lo, x, y).
Axes of the slice: x: 4, y: 8, z: 8 (z_hi: 4, z_lo: 2; z = z_hi * 2 + z_lo), core: 2. Of those that a mesh axis runs over, the one named last changes fastest.
Arguments:
- inputs: bfloat16 [2048, 4096], P('dp'), may hold values from -6 to 6
- upstream: bfloat16 [2048, 4096], P('dp'), may hold values from -6 to 6
- eig_tiles: bfloat16 [64, 8, 2, 128, 128], P('mp'), may hold values from -0.09375 to 0.09375
- eigvals: float32 [4096], replicated, may hold values from 0.25 to 4
Outputs:
- grad_t: bfloat16 [4096, 2048], P('mp', 'dp')
The draws below stay inside these ranges and needn't reach their ends.
All inputs are finite; a program needn't handle non-finite values.
Results may differ from the reference program's by a relative error of at most 0.013.
Values may be sent and summed in bfloat16 or wider, within the bound.
No kernel may reach another device: no remote copies, remote signals or barrier semaphores. Data moves between devices by JAX's collectives and lax.ppermute only.
A program may use at most 64 MiB of HBM per device.

```python
import math
import jax
import jax.numpy as jnp
from jax import lax

D = 4096
TILE = 128
PR = 4
PC = 16
RT = 8
CT = 2
TOKENS = 2048
N_MP = 64


def block_levels(stream_key, extent, split, low, high):
    factor_of = 1.0
    for axis_at, shards_of in split:
        steps = jax.random.uniform(jax.random.fold_in(jax.random.fold_in(stream_key, 6), axis_at), (shards_of,), jnp.float32, low / len(split), high / len(split))
        factor_of = factor_of * jnp.repeat(jnp.exp(steps), extent[axis_at] // shards_of).reshape((-1,) + (1,) * (len(extent) - 1 - axis_at))
    return factor_of


def normal_values(rng, extent, deviation, reach, split=(), kind=jnp.bfloat16):
    result = jax.random.normal(rng, extent, jnp.float32) * deviation
    if len(split) > 0:
        result = block_levels(rng, extent, split, -0.22, 0.18) * result
    return jnp.clip(result, min=-reach, max=reach).astype(kind)


def setup_inputs(seed: int = 0) -> dict:
    streams_of = jax.random.split(jax.random.key(seed), 5)
    inputs = normal_values(streams_of[0], (TOKENS, D), 1.0, 6.0, ((0, 8),))
    upstream = normal_values(streams_of[1], (TOKENS, D), 1.0, 6.0, ((0, 8),))
    eig_tiles = normal_values(streams_of[2], (N_MP, RT, CT, TILE, TILE), D ** -0.5, 0.09375, ((0, 64),))
    eigvals = jnp.clip(jnp.exp(jax.random.uniform(streams_of[3], (D,), jnp.float32, math.log(0.25), math.log(4.0))), 0.25, 4.0)
    return dict(inputs=inputs, upstream=upstream, eig_tiles=eig_tiles, eigvals=eigvals)


def reference(inputs, upstream, eig_tiles, eigvals):
    layout = eig_tiles.reshape(PR, PC, RT, CT, TILE, TILE)
    basis = jnp.transpose(layout, (2, 0, 4, 3, 1, 5)).reshape(D, D)
    proj_in = jnp.dot(inputs, basis, preferred_element_type=jnp.float32).astype(jnp.bfloat16)
    proj_up = jnp.dot(upstream, basis, preferred_element_type=jnp.float32).astype(jnp.bfloat16)
    gram = jnp.dot(proj_in.T, proj_up, preferred_element_type=jnp.float32)
    sym = 0.5 * (gram + gram.T)
    root = jnp.sqrt(eigvals)
    kernel = -1.0 / (root[:, None] * root[None, :] * (root[:, None] + root[None, :]))
    weighted = (kernel * sym).astype(jnp.bfloat16)
    mixed = jnp.dot(proj_in, weighted, preferred_element_type=jnp.float32)
    update = (proj_up.astype(jnp.float32) / root[None, :] + 2.0 / TOKENS * mixed).astype(jnp.bfloat16)
    grad_t = lax.dot_general(basis, update, (((1,), (1,)), ((), ())), preferred_element_type=jnp.float32)
    return grad_t.astype(jnp.bfloat16)
```

```python
import functools

import jax
import jax.numpy as jnp
from jax import lax
from jax.experimental import pallas as pl
from jax.experimental.pallas import tpu as pltpu
from jax.sharding import Mesh
from jax.sharding import PartitionSpec as P

F32 = jnp.float32
BF16 = jnp.bfloat16
AXES = ("zh", "core", "zl", "xh", "xl", "y")
SIZES = (4, 2, 2, 2, 2, 8)
ROWS = ("zl", "xh")
PLANE = ("zl", "xh", "xl")
COLS = ("xl", "zl", "xh")


def vmem(n):
    return [pl.BlockSpec(memory_space=pltpu.VMEM)] * n


def project_kernel(r_ref, x_ref, y_ref, eig_ref, out_ref, xs, sems):
    steps = eig_ref.shape[0]
    grid_rows = x_ref.shape[1] // (steps * 128)
    r = r_ref[0]

    def copy(s, la):
        src = x_ref if s == 0 else y_ref
        start = pl.multiple_of((la * grid_rows + r) * 128, 128)
        return pltpu.make_async_copy(
            src.at[:, pl.ds(start, 128)], xs.at[s, :, pl.ds(la * 128, 128)], sems.at[s, la]
        )

    for s in range(2):
        for la in range(steps):
            copy(s, la).start()
    lb_n = eig_ref.shape[1]
    basis = jnp.concatenate(
        [eig_ref[:, lb].reshape(steps * 128, 128) for lb in range(lb_n)], 1
    )
    for s in range(2):
        for la in range(steps):
            copy(s, la).wait()
        part = jnp.dot(xs[s], basis, preferred_element_type=F32)
        turned = part.T.astype(BF16)
        out_ref[:, s] = turned.reshape(out_ref.shape[0], out_ref.shape[2], out_ref.shape[3])


def project(r, inputs, upstream, eig):
    tokens = inputs.shape[0]
    steps = eig.shape[0]
    return pl.pallas_call(
        project_kernel,
        out_shape=jax.ShapeDtypeStruct((4, 2, 64, tokens), BF16),
        in_specs=[
            pl.BlockSpec(memory_space=pltpu.SMEM),
            pl.BlockSpec(memory_space=pl.ANY),
            pl.BlockSpec(memory_space=pl.ANY),
            pl.BlockSpec(memory_space=pltpu.VMEM),
        ],
        out_specs=pl.BlockSpec(memory_space=pltpu.VMEM),
        scratch_shapes=[
            pltpu.VMEM((2, tokens, steps * 128), BF16),
            pltpu.SemaphoreType.DMA((2, steps)),
        ],
        name="project",
    )(r, inputs, upstream, eig)


def gram_kernel(core_ref, b_ref, a_ref, keep_ref, send_ref):
    mine = core_ref[0]
    n = a_ref.shape[0] * a_ref.shape[2]
    tokens = a_ref.shape[3]
    half = b_ref.shape[0] // 2
    right_in = a_ref[:, 0].reshape(n, tokens)
    right_up = a_ref[:, 1].reshape(n, tokens)
    over = (((1,), (1,)), ((), ()))
    for out_ref, which in ((send_ref, 1 - mine), (keep_ref, mine)):
        left = b_ref[pl.ds(which * half, half)]
        left_in = left[:, 0].reshape(half * 64, tokens)
        left_up = left[:, 1].reshape(half * 64, tokens)
        block = lax.dot_general(left_in, right_up, over, preferred_element_type=F32)
        block += lax.dot_general(left_up, right_in, over, preferred_element_type=F32)
        out_ref[...] = block.astype(BF16)


def gram_of(core, left, right):
    n = right.shape[0] * right.shape[2]
    shape = jax.ShapeDtypeStruct((left.shape[0] // 2 * 64, n), BF16)
    return pl.pallas_call(
        gram_kernel,
        out_shape=(shape, shape),
        in_specs=[pl.BlockSpec(memory_space=pltpu.SMEM)] + vmem(2),
        out_specs=tuple(vmem(2)),
        name="gram",
    )(core, left, right)


def on_device(inputs, upstream, eig_tiles, eigvals):
    zl, xh, xl, y = (lax.axis_index(a) for a in ("zl", "xh", "xl", "y"))
    zh, core = lax.axis_index("zh"), lax.axis_index("core")
    tokens = inputs.shape[0]
    eig = eig_tiles[0]
    core_at = core.reshape(1).astype(jnp.int32)

    by_b = lax.dynamic_index_in_dim(eigvals.reshape(2, 2, 8, 128), y, 2, keepdims=False)
    lam_b = jnp.transpose(by_b, (1, 0, 2)).reshape(8, 64)
    cube = jnp.transpose(eigvals.reshape(2, 2, 8, 2, 64), (0, 3, 1, 2, 4)).reshape(8, 8, 64)
    lam_a = lax.dynamic_index_in_dim(cube, zl * 4 + xh * 2 + xl, 0, keepdims=False)
    lam_own = lax.dynamic_index_in_dim(lam_a, y, 0, keepdims=False)
    lam_part = lax.dynamic_index_in_dim(lam_b, core * 4 + zh, 0, keepdims=False)

    parts = project((zl * 2 + xh).reshape(1).astype(jnp.int32), inputs, upstream, eig)
    got = lax.all_to_all(parts, ROWS, 0, 0, tiled=True)
    own = jnp.sum(got.astype(F32), 0).astype(BF16)
    copies = jnp.broadcast_to(own[None], (8, *own.shape))
    left = lax.all_to_all(copies, COLS, 0, 0, tiled=True)
    right = lax.all_to_all(copies, "y", 0, 0, tiled=True)
    rows = lax.all_to_all(eig, PLANE, 0, 0, tiled=True)
    basis_rows = jnp.transpose(rows.reshape(4, 2, 2, 128, 128), (0, 3, 1, 2, 4)).reshape(512, 512)

    keep, send = gram_of(core_at, left, right)
    swap = [(0, 1), (1, 0)]
    other = lax.ppermute(send, "core", swap)
    pair = (keep.astype(F32) + other.astype(F32)).astype(BF16).reshape(4, 64, 512)
    share = jnp.sum(lax.all_to_all(pair, "zh", 0, 0, tiled=True).astype(F32), 0)
    s_b = jnp.sqrt(lam_part)[:, None]
    s_a = jnp.sqrt(lam_a.reshape(512))[None, :]
    kernel = -1.0 / (s_b * s_a * (s_b + s_a))
    part = (kernel * (0.5 * share)).astype(BF16)
    mine = lax.all_to_all(jnp.broadcast_to(part[None], (4, 64, 512)), "zh", 0, 0, tiled=True)
    theirs = lax.ppermute(mine, "core", swap)
    first = core == 0
    weighted = jnp.concatenate(
        [jnp.where(first, mine, theirs), jnp.where(first, theirs, mine)], 0
    ).reshape(512, 512)
    proj_in = right[:, 0].reshape(512, tokens)
    mixed_part = jnp.dot(weighted, proj_in, preferred_element_type=F32).astype(BF16)
    mixed = jnp.sum(
        lax.all_to_all(mixed_part.reshape(8, 64, tokens), COLS, 0, 0, tiled=True).astype(F32), 0
    )
    factor = 2.0 / (8 * tokens)
    update = (own[1].astype(F32) / jnp.sqrt(lam_own)[:, None] + factor * mixed).astype(BF16)
    every = lax.all_to_all(jnp.broadcast_to(update[None], (8, 64, tokens)), COLS, 0, 0, tiled=True)
    grad_part = jnp.dot(basis_rows, every.reshape(512, tokens), preferred_element_type=F32)
    blocks = lax.all_to_all(grad_part.astype(BF16).reshape(8, 64, tokens), "y", 0, 0, tiled=True)
    return jnp.sum(blocks.astype(F32), 0).astype(BF16)


def solution(mesh):
    grid = Mesh(mesh.devices.reshape(SIZES), AXES)
    dp, mp = AXES[:2], AXES[2:]
    return jax.shard_map(
        on_device,
        mesh=grid,
        in_specs=(P(dp, None), P(dp, None), P(mp, None, None, None, None), P()),
        out_specs=P(mp, dp),
        check_vma=False,
    )
```

```python
import jax
import jax.numpy as jnp
from jax import lax
from jax.experimental import pallas as pl
from jax.experimental.pallas import tpu as pltpu
from jax.sharding import Mesh
from jax.sharding import PartitionSpec as P

F32 = jnp.float32
BF16 = jnp.bfloat16
AXES = ("zh", "core", "zl", "xh", "xl", "y")
SIZES = (4, 2, 2, 2, 2, 8)
ROWS = ("zl", "xh")
PLANE = ("zl", "xh", "xl")
COLS = ("xl", "zl", "xh")


def vmem(n):
    return [pl.BlockSpec(memory_space=pltpu.VMEM)] * n


def project_kernel(r_ref, x_ref, y_ref, eig_ref, *refs):
    *out_refs, blocks, xs, sems = refs
    steps = eig_ref.shape[0]
    grid_rows = x_ref.shape[1] // (steps * 128)
    r = r_ref[0]

    def copy(s, la):
        src = x_ref if s == 0 else y_ref
        start = pl.multiple_of((la * grid_rows + r) * 128, 128)
        return pltpu.make_async_copy(
            src.at[:, pl.ds(start, 128)], xs.at[s, :, pl.ds(la * 128, 128)], sems.at[s, la]
        )

    for s in range(2):
        for la in range(steps):
            copy(s, la).start()
    lb_n = eig_ref.shape[1]
    basis = jnp.concatenate(
        [eig_ref[:, lb].reshape(steps * 128, 128) for lb in range(lb_n)], 1
    )
    for s in range(2):
        for la in range(steps):
            copy(s, la).wait()
        part = jnp.dot(xs[s], basis, preferred_element_type=F32)
        blocks[:, s] = part.T.astype(BF16).reshape(blocks.shape[0], *blocks.shape[2:])
    for k, out_ref in enumerate(out_refs):
        out_ref[...] = blocks[r ^ k]


def project(r, inputs, upstream, eig):
    tokens = inputs.shape[0]
    steps = eig.shape[0]
    return pl.pallas_call(
        project_kernel,
        out_shape=(jax.ShapeDtypeStruct((2, 64, tokens), BF16),) * 4,
        in_specs=[
            pl.BlockSpec(memory_space=pltpu.SMEM),
            pl.BlockSpec(memory_space=pl.ANY),
            pl.BlockSpec(memory_space=pl.ANY),
            pl.BlockSpec(memory_space=pltpu.VMEM),
        ],
        out_specs=tuple(vmem(4)),
        scratch_shapes=[
            pltpu.VMEM((4, 2, 64, tokens), BF16),
            pltpu.VMEM((2, tokens, steps * 128), BF16),
            pltpu.SemaphoreType.DMA((2, steps)),
        ],
        name="project",
    )(r, inputs, upstream, eig)


def spread_kernel(*refs):
    *parts, _, own_ref, copies_ref = refs
    total = parts[0][...].astype(F32)
    for part in parts[1:]:
        total += part[...].astype(F32)
    own = total.astype(BF16)
    own_ref[...] = own
    for k in range(copies_ref.shape[0]):
        copies_ref[k] = own


def spread(parts, after):
    shape = parts[0].shape
    return pl.pallas_call(
        spread_kernel,
        out_shape=(
            jax.ShapeDtypeStruct(shape, BF16),
            jax.ShapeDtypeStruct((8, *shape), BF16),
        ),
        in_specs=vmem(len(parts)) + [pl.BlockSpec(memory_space=pl.ANY)],
        out_specs=tuple(vmem(2)),
        name="spread",
    )(*parts, after)


def gram_kernel(at_ref, own_ref, one_ref, two_ref, four_ref, a_ref, keep_ref, send_ref, left):
    mine, here = at_ref[0], at_ref[1]
    n = a_ref.shape[0] * a_ref.shape[2]
    tokens = a_ref.shape[3]
    half = left.shape[0] // 2
    pieces = [own_ref, one_ref] + [two_ref.at[i] for i in range(2)]
    pieces += [four_ref.at[i] for i in range(4)]
    for k, piece in enumerate(pieces):
        left[here ^ ((k & 1) * 4 + (k >> 1))] = piece[...]
    right_in = a_ref[:, 0].reshape(n, tokens)
    right_up = a_ref[:, 1].reshape(n, tokens)
    over = (((1,), (1,)), ((), ()))
    for out_ref, which in ((send_ref, 1 - mine), (keep_ref, mine)):
        rows = left[pl.ds(which * half, half)]
        left_in = rows[:, 0].reshape(half * 64, tokens)
        left_up = rows[:, 1].reshape(half * 64, tokens)
        block = lax.dot_general(left_in, right_up, over, preferred_element_type=F32)
        block += lax.dot_general(left_up, right_in, over, preferred_element_type=F32)
        out_ref[...] = block.astype(BF16)


def gram_of(at, pieces, right):
    n = right.shape[0] * right.shape[2]
    shape = jax.ShapeDtypeStruct((4 * 64, n), BF16)
    return pl.pallas_call(
        gram_kernel,
        out_shape=(shape, shape),
        in_specs=[pl.BlockSpec(memory_space=pltpu.SMEM)] + vmem(5),
        out_specs=tuple(vmem(2)),
        scratch_shapes=[pltpu.VMEM(right.shape, BF16)],
        name="gram",
    )(at, *pieces, right)


def on_device(inputs, upstream, eig_tiles, eigvals):
    zl, xh, xl, y = (lax.axis_index(a) for a in ("zl", "xh", "xl", "y"))
    zh, core = lax.axis_index("zh"), lax.axis_index("core")
    tokens = inputs.shape[0]
    eig = eig_tiles[0]

    by_b = lax.dynamic_index_in_dim(eigvals.reshape(2, 2, 8, 128), y, 2, keepdims=False)
    lam_b = jnp.transpose(by_b, (1, 0, 2)).reshape(8, 64)
    cube = jnp.transpose(eigvals.reshape(2, 2, 8, 2, 64), (0, 3, 1, 2, 4)).reshape(8, 8, 64)
    lam_a = lax.dynamic_index_in_dim(cube, zl * 4 + xh * 2 + xl, 0, keepdims=False)
    lam_own = lax.dynamic_index_in_dim(lam_a, y, 0, keepdims=False)
    lam_part = lax.dynamic_index_in_dim(lam_b, core * 4 + zh, 0, keepdims=False)

    rows = lax.all_to_all(eig, PLANE, 0, 0, tiled=True)
    r = zl * 2 + xh
    parts = project(r.reshape(1).astype(jnp.int32), inputs, upstream, eig)
    got = [parts[0]]
    for k in range(1, 4):
        got.append(lax.ppermute(parts[k], ROWS, [(i, i ^ k) for i in range(4)]))
    own, copies = spread(got, rows)
    right = lax.all_to_all(copies, "y", 0, 0, tiled=True)
    swap = [(0, 1), (1, 0)]
    one = lax.ppermute(own, "xl", swap)
    pair_of = jnp.stack([own, one])
    two = lax.ppermute(pair_of, "xh", swap)
    four = lax.ppermute(jnp.concatenate([pair_of, two]), "zl", swap)
    basis_rows = jnp.transpose(rows.reshape(4, 2, 2, 128, 128), (0, 3, 1, 2, 4)).reshape(512, 512)

    at = jnp.stack([core, xl * 4 + r]).astype(jnp.int32)
    keep, send = gram_of(at, (own, one, two, four), right)
    other = lax.ppermute(send, "core", swap)
    pair = (keep.astype(F32) + other.astype(F32)).astype(BF16).reshape(4, 64, 512)
    share = jnp.sum(lax.all_to_all(pair, "zh", 0, 0, tiled=True).astype(F32), 0)
    s_b = jnp.sqrt(lam_part)[:, None]
    s_a = jnp.sqrt(lam_a.reshape(512))[None, :]
    kernel = -1.0 / (s_b * s_a * (s_b + s_a))
    part = (kernel * (0.5 * share)).astype(BF16)
    mine = lax.all_to_all(jnp.broadcast_to(part[None], (4, 64, 512)), "zh", 0, 0, tiled=True)
    theirs = lax.ppermute(mine, "core", swap)
    first = core == 0
    weighted = jnp.concatenate(
        [jnp.where(first, mine, theirs), jnp.where(first, theirs, mine)], 0
    ).reshape(512, 512)
    proj_in = right[:, 0].reshape(512, tokens)
    mixed_part = jnp.dot(weighted, proj_in, preferred_element_type=F32).astype(BF16)
    mixed = jnp.sum(
        lax.all_to_all(mixed_part.reshape(8, 64, tokens), COLS, 0, 0, tiled=True).astype(F32), 0
    )
    factor = 2.0 / (8 * tokens)
    update = (own[1].astype(F32) / jnp.sqrt(lam_own)[:, None] + factor * mixed).astype(BF16)
    every = lax.all_to_all(jnp.broadcast_to(update[None], (8, 64, tokens)), COLS, 0, 0, tiled=True)
    grad_part = jnp.dot(basis_rows, every.reshape(512, tokens), preferred_element_type=F32)
    blocks = lax.all_to_all(grad_part.astype(BF16).reshape(8, 64, tokens), "y", 0, 0, tiled=True)
    return jnp.sum(blocks.astype(F32), 0).astype(BF16)


def solution(mesh):
    grid = Mesh(mesh.devices.reshape(SIZES), AXES)
    dp, mp = AXES[:2], AXES[2:]
    return jax.shard_map(
        on_device,
        mesh=grid,
        in_specs=(P(dp, None), P(dp, None), P(mp, None, None, None, None), P()),
        out_specs=P(mp, dp),
        check_vma=False,
    )
```

```python
import jax
import jax.numpy as jnp
from jax import lax
from jax.experimental import pallas as pl
from jax.experimental.pallas import tpu as pltpu
from jax.sharding import Mesh
from jax.sharding import PartitionSpec as P

F32 = jnp.float32
BF16 = jnp.bfloat16
AXES = ("zh", "core", "zl", "xh", "xl", "y")
SIZES = (4, 2, 2, 2, 2, 8)
ROWS = ("zl", "xh")
COLS = ("xl", "zl", "xh")
PLANE = ("zl", "xh", "xl")
LINE = ("xh", "xl")
SWAP = [(0, 1), (1, 0)]

IN_SMEM = pl.BlockSpec(memory_space=pltpu.SMEM)
ANYWHERE = pl.BlockSpec(memory_space=pl.ANY)
IN_VMEM = pl.BlockSpec(memory_space=pltpu.VMEM)


def call(kernel, scalars, arrays, outs, scratch=(), after=()):
    held = [pltpu.with_memory_space_constraint(a, pltpu.VMEM) for a in arrays]
    single = not isinstance(outs, (list, tuple))
    shapes = [outs] if single else outs
    got = pl.pallas_call(
        kernel,
        out_shape=[pltpu.VMEM(s, d) for s, d in shapes_of(shapes)],
        in_specs=[IN_SMEM] * len(scalars) + [IN_VMEM] * len(held) + [ANYWHERE] * len(after),
        out_specs=[IN_VMEM] * len(shapes),
        scratch_shapes=list(scratch),
    )(*scalars, *held, *after)
    return got[0] if single else got


def shapes_of(outs):
    return [(o.shape, o.dtype) for o in outs]


def out(dtype, *shape):
    return jax.ShapeDtypeStruct(shape, dtype)


def project_kernel(r_ref, x_ref, y_ref, eig_ref, out_ref, xs, tiles, sems, tile_sem):
    steps = eig_ref.shape[0]
    grid_rows = x_ref.shape[1] // (steps * 128)
    r = r_ref[0]

    def copy(s, la):
        src = x_ref if s == 0 else y_ref
        start = pl.multiple_of((la * grid_rows + r) * 128, 128)
        return pltpu.make_async_copy(
            src.at[:, pl.ds(start, 128)], xs.at[s, :, pl.ds(la * 128, 128)], sems.at[s, la]
        )

    load = pltpu.make_async_copy(eig_ref, tiles, tile_sem)
    load.start()
    for s in range(2):
        for la in range(steps):
            copy(s, la).start()
    load.wait()
    basis = jnp.concatenate(
        [tiles[:, lb].reshape(steps * 128, 128) for lb in range(tiles.shape[1])], 1
    )
    for s in range(2):
        for la in range(steps):
            copy(s, la).wait()
        part = jnp.dot(xs[s], basis, preferred_element_type=F32)
        turned = part.T.astype(BF16)
        out_ref[:, s] = turned.reshape(out_ref.shape[0], *out_ref.shape[2:])


def project(r, inputs, upstream, eig):
    tokens = inputs.shape[0]
    steps = eig.shape[0]
    return pl.pallas_call(
        project_kernel,
        out_shape=pltpu.VMEM((4, 2, 64, tokens), BF16),
        in_specs=[IN_SMEM, ANYWHERE, ANYWHERE, ANYWHERE],
        out_specs=IN_VMEM,
        scratch_shapes=[
            pltpu.VMEM((2, tokens, steps * 128), BF16),
            pltpu.VMEM(eig.shape, BF16),
            pltpu.SemaphoreType.DMA((2, steps)),
            pltpu.SemaphoreType.DMA,
        ],
        name="project",
    )(r, inputs, upstream, eig)


def spread_kernel(parts_ref, own_ref, copies_ref):
    total = parts_ref[0].astype(F32)
    for k in range(1, parts_ref.shape[0]):
        total += parts_ref[k].astype(F32)
    own = total.astype(BF16)
    own_ref[...] = own
    for k in range(copies_ref.shape[0]):
        copies_ref[k] = own


def gram_kernel(at_ref, *refs):
    pieces, (a_ref, *rest) = refs[:8], refs[8:]
    out_ref, left = rest[-2:]
    half, here = at_ref[0], at_ref[1]
    n = a_ref.shape[0] * a_ref.shape[2]
    tokens = a_ref.shape[3]
    apart = half ^ (here // 4)
    for group in range(2):

        @pl.when(apart == group)
        def _():
            for k in range(4):
                left[(here % 4) ^ k] = pieces[group * 4 + k][...]

    over = (((1,), (1,)), ((), ()))
    right_in = a_ref[:, 0].reshape(n, tokens)
    right_up = a_ref[:, 1].reshape(n, tokens)
    block = lax.dot_general(
        left[:, 0].reshape(256, tokens), right_up, over, preferred_element_type=F32
    )
    block += lax.dot_general(
        left[:, 1].reshape(256, tokens), right_in, over, preferred_element_type=F32
    )
    out_ref[...] = block.astype(BF16)


def add_kernel(a_ref, b_ref, out_ref):
    total = a_ref[...].astype(F32) + b_ref[...].astype(F32)
    out_ref[...] = total.astype(BF16).reshape(out_ref.shape)


def weigh_kernel(parts_ref, rows_ref, cols_ref, *rest):
    out_ref = rest[-1]
    share = parts_ref[0].astype(F32)
    for k in range(1, parts_ref.shape[0]):
        share += parts_ref[k].astype(F32)
    s_b = jnp.sqrt(rows_ref[...])
    s_a = jnp.sqrt(cols_ref[...])
    kernel = -1.0 / (s_b * s_a * (s_b + s_a))
    part = (kernel * (0.5 * share)).astype(BF16)
    for k in range(out_ref.shape[0]):
        out_ref[k] = part


def mix_kernel(core_ref, mine_ref, theirs_ref, a_ref, out_ref):
    core = core_ref[0]
    tokens = a_ref.shape[3]
    proj_in = a_ref[:, 0].reshape(-1, tokens)
    for half, ref in ((core, mine_ref), (1 - core, theirs_ref)):
        part = jnp.dot(ref[...].reshape(256, -1), proj_in, preferred_element_type=F32)
        out_ref[pl.ds(half * 4, 4)] = part.astype(BF16).reshape(4, 64, tokens)


def update_kernel(factor, parts_ref, own_ref, lam_ref, out_ref):
    mixed = parts_ref[0].astype(F32)
    for k in range(1, parts_ref.shape[0]):
        mixed += parts_ref[k].astype(F32)
    update = own_ref[1].astype(F32) / jnp.sqrt(lam_ref[...]) + factor * mixed
    update = update.astype(BF16)
    for k in range(out_ref.shape[0]):
        out_ref[k] = update


def assemble_kernel(at_ref, pair_ref, *refs):
    xh, xl = at_ref[0], at_ref[1]
    *got_refs, out_ref = refs
    here = xh * 2 + xl
    for k in range(4):
        piece = pair_ref.at[:, here] if k == 0 else got_refs[k - 1]
        there_h, there_l = xh ^ (k >> 1), xl ^ (k & 1)
        for zl in range(2):
            block = jnp.concatenate([piece[zl, 0], piece[zl, 1]], 1)
            cols = pl.ds(pl.multiple_of(there_l * 256, 256), 256)
            out_ref[zl * 2 + there_h, :, cols] = block


def finish_kernel(basis_ref, every_ref, out_ref):
    tokens = every_ref.shape[2]
    part = jnp.dot(
        basis_ref[...].reshape(512, 512),
        every_ref[...].reshape(512, tokens),
        preferred_element_type=F32,
    )
    out_ref[...] = part.astype(BF16).reshape(out_ref.shape)


def scalars(*values):
    return jnp.stack(values).astype(jnp.int32)


def on_device(inputs, upstream, eig_tiles, eigvals):
    zl, xh, xl, y = (lax.axis_index(a) for a in ("zl", "xh", "xl", "y"))
    zh, core = lax.axis_index("zh"), lax.axis_index("core")
    tokens = inputs.shape[0]
    eig = eig_tiles[0]
    r = zl * 2 + xh
    here = xl * 4 + r

    by_b = lax.dynamic_index_in_dim(eigvals.reshape(2, 2, 8, 128), y, 2, keepdims=False)
    lam_b = jnp.transpose(by_b, (1, 0, 2)).reshape(8, 64)
    cube = jnp.transpose(eigvals.reshape(2, 2, 8, 2, 64), (0, 3, 1, 2, 4)).reshape(8, 8, 64)
    lam_a = lax.dynamic_index_in_dim(cube, r * 2 + xl, 0, keepdims=False)
    lam_own = lax.dynamic_index_in_dim(lam_a, y, 0, keepdims=False).reshape(64, 1)
    lam_rows = lax.dynamic_index_in_dim(lam_b, core * 4 + zh, 0, keepdims=False).reshape(64, 1)
    lam_cols = lam_a.reshape(1, 512)

    parts = project(scalars(r), inputs, upstream, eig)
    got = lax.all_to_all(parts, ROWS, 0, 0, tiled=True)
    own, copies = call(
        spread_kernel, (), (got,), (out(BF16, 2, 64, tokens), out(BF16, 8, 2, 64, tokens))
    )
    right = lax.all_to_all(copies, "y", 0, 0, tiled=True)
    pieces = [own]
    for k in range(1, 8):
        p = (k >> 1) * 2 % 4 * 2 + (k & 1) * 2 + (k >> 2)
        pieces.append(lax.ppermute(own, PLANE, [(i, i ^ p) for i in range(8)]))

    halves = eig.reshape(2, 4, 2, 128, 128)
    away = lax.dynamic_index_in_dim(halves, 1 - zl, 0, keepdims=False)
    kept = lax.dynamic_index_in_dim(halves, zl, 0, keepdims=False)
    came = lax.ppermute(away, "zl", SWAP)
    pair = jnp.where(zl == 0, jnp.stack([kept, came]), jnp.stack([came, kept]))

    half_block = out(BF16, 256, 512)
    room = [pltpu.VMEM((4, 2, 64, tokens), BF16)]
    send = call(
        gram_kernel, (scalars(1 - core, here),), (*pieces, right), half_block, room, (came,)
    )
    other = lax.ppermute(send, "core", SWAP)
    keep = call(gram_kernel, (scalars(core, here),), (*pieces, right), half_block, room)
    both = call(add_kernel, (), (keep, other), out(BF16, 4, 64, 512))

    line = xh * 2 + xl
    near = []
    for k in range(1, 4):
        chunk = lax.dynamic_index_in_dim(pair, line ^ k, 1, keepdims=False)
        near.append(lax.ppermute(chunk, LINE, [(i, i ^ k) for i in range(4)]))

    shares = lax.all_to_all(both, "zh", 0, 0, tiled=True)
    part = call(
        weigh_kernel, (), (shares, lam_rows, lam_cols), out(BF16, 4, 64, 512), (), tuple(near)
    )
    mine = lax.all_to_all(part, "zh", 0, 0, tiled=True)
    theirs = lax.ppermute(mine, "core", SWAP)
    mixed_part = call(mix_kernel, (scalars(core),), (mine, theirs, right), out(BF16, 8, 64, tokens))
    basis_rows = call(assemble_kernel, (scalars(xh, xl),), (pair, *near), out(BF16, 4, 128, 512))
    mixed = lax.all_to_all(mixed_part, COLS, 0, 0, tiled=True)
    factor = 2.0 / (8 * tokens)
    update = call(
        lambda *refs: update_kernel(factor, *refs),
        (),
        (mixed, own, lam_own),
        out(BF16, 8, 64, tokens),
    )
    every = lax.all_to_all(update, COLS, 0, 0, tiled=True)
    grad_part = call(finish_kernel, (), (basis_rows, every), out(BF16, 8, 64, tokens))
    blocks = lax.all_to_all(grad_part, "y", 0, 0, tiled=True)
    return jnp.sum(blocks.astype(F32), 0).astype(BF16)


def solution(mesh):
    grid = Mesh(mesh.devices.reshape(SIZES), AXES)
    dp, mp = AXES[:2], AXES[2:]
    return jax.shard_map(
        on_device,
        mesh=grid,
        in_specs=(P(dp, None), P(dp, None), P(mp, None, None, None, None), P()),
        out_specs=P(mp, dp),
        check_vma=False,
    )
```

```python
import jax
import jax.numpy as jnp
from jax import lax
from jax.experimental import pallas as pl
from jax.experimental.pallas import tpu as pltpu
from jax.sharding import Mesh
from jax.sharding import PartitionSpec as P

F32 = jnp.float32
BF16 = jnp.bfloat16
AXES = ("zh", "core", "zl", "xh", "xl", "y")
SIZES = (4, 2, 2, 2, 2, 8)
ROWS = ("zl", "xh")
COLS = ("xl", "zl", "xh")
SWAP = [(0, 1), (1, 0)]

ANYWHERE = pl.BlockSpec(memory_space=pl.ANY)
IN_VMEM = pl.BlockSpec(memory_space=pltpu.VMEM)


def call(kernel, arrays, outs, scratch=()):
    held = [pltpu.with_memory_space_constraint(a, pltpu.VMEM) for a in arrays]
    single = not isinstance(outs, (list, tuple))
    shapes = [outs] if single else outs
    got = pl.pallas_call(
        kernel,
        out_shape=[pltpu.VMEM(s, d) for s, d in shapes_of(shapes)],
        in_specs=[IN_VMEM] * len(held),
        out_specs=[IN_VMEM] * len(shapes),
        scratch_shapes=list(scratch),
    )(*held)
    return got[0] if single else got


def shapes_of(outs):
    return [(o.shape, o.dtype) for o in outs]


def out(dtype, *shape):
    return jax.ShapeDtypeStruct(shape, dtype)


def project_kernel(x_ref, y_ref, eig_ref, out_ref, xs, tiles, sems, tile_sem):
    steps = eig_ref.shape[0]
    grid_rows = x_ref.shape[1] // (steps * 128)
    r = lax.axis_index("zl") * 2 + lax.axis_index("xh")

    def copy(s, la):
        src = x_ref if s == 0 else y_ref
        start = pl.multiple_of((la * grid_rows + r) * 128, 128)
        return pltpu.make_async_copy(
            src.at[:, pl.ds(start, 128)], xs.at[s, :, pl.ds(la * 128, 128)], sems.at[s, la]
        )

    load = pltpu.make_async_copy(eig_ref, tiles, tile_sem)
    load.start()
    for s in range(2):
        for la in range(steps):
            copy(s, la).start()
    load.wait()
    basis = jnp.concatenate(
        [tiles[:, lb].reshape(steps * 128, 128) for lb in range(tiles.shape[1])], 1
    )
    for s in range(2):
        for la in range(steps):
            copy(s, la).wait()
        part = jnp.dot(xs[s], basis, preferred_element_type=F32)
        turned = part.T.astype(BF16)
        out_ref[:, s] = turned.reshape(out_ref.shape[0], *out_ref.shape[2:])


def project(inputs, upstream, eig):
    tokens = inputs.shape[0]
    steps = eig.shape[0]
    return pl.pallas_call(
        project_kernel,
        out_shape=pltpu.VMEM((4, 2, 64, tokens), BF16),
        in_specs=[ANYWHERE] * 3,
        out_specs=IN_VMEM,
        scratch_shapes=[
            pltpu.VMEM((2, tokens, steps * 128), BF16),
            pltpu.VMEM(eig.shape, BF16),
            pltpu.SemaphoreType.DMA((2, steps)),
            pltpu.SemaphoreType.DMA,
        ],
        name="project",
    )(inputs, upstream, eig)


def spread_kernel(parts_ref, own_ref, copies_ref):
    total = parts_ref[0].astype(F32)
    for k in range(1, parts_ref.shape[0]):
        total += parts_ref[k].astype(F32)
    own = total.astype(BF16)
    own_ref[...] = own
    for k in range(copies_ref.shape[0]):
        copies_ref[k] = own


def gram_kernel(which):
    def kernel(b_ref, a_ref, out_ref):
        half = lax.axis_index("core") ^ which
        n = a_ref.shape[0] * a_ref.shape[2]
        tokens = a_ref.shape[3]
        over = (((1,), (1,)), ((), ()))
        left = b_ref[pl.ds(half * 4, 4)]
        block = lax.dot_general(
            left[:, 0].reshape(256, tokens),
            a_ref[:, 1].reshape(n, tokens),
            over,
            preferred_element_type=F32,
        )
        block += lax.dot_general(
            left[:, 1].reshape(256, tokens),
            a_ref[:, 0].reshape(n, tokens),
            over,
            preferred_element_type=F32,
        )
        out_ref[...] = block.astype(BF16)

    return kernel


def add_kernel(a_ref, b_ref, out_ref):
    total = a_ref[...].astype(F32) + b_ref[...].astype(F32)
    out_ref[...] = total.astype(BF16).reshape(out_ref.shape)


def roots_kernel(*refs):
    for k in range(3):
        refs[3 + k][...] = jnp.sqrt(refs[k][...])


def weigh_kernel(parts_ref, rows_ref, cols_ref, out_ref):
    share = parts_ref[0].astype(F32)
    for k in range(1, parts_ref.shape[0]):
        share += parts_ref[k].astype(F32)
    s_b, s_a = rows_ref[...], cols_ref[...]
    kernel = -1.0 / (s_b * s_a * (s_b + s_a))
    part = (kernel * (0.5 * share)).astype(BF16)
    for k in range(out_ref.shape[0]):
        out_ref[k] = part


def mix_kernel(half_ref, a_ref, other_ref, out_ref):
    core = lax.axis_index("core")
    tokens = a_ref.shape[3]
    weights = half_ref[...].reshape(256, -1)
    for to, proj_in in ((core, a_ref[:, 0]), (core ^ 1, other_ref[...])):
        part = jnp.dot(weights, proj_in.reshape(-1, tokens), preferred_element_type=F32)
        part = part.astype(BF16)
        for r in range(4):
            for xl in range(2):
                row = r * 64 + xl * 32
                out_ref[to, xl, r] = part[row : row + 32]


def update_kernel(factor, parts_ref, left_ref, root_ref, out_ref):
    zl, xh, xl = lax.axis_index("zl"), lax.axis_index("xh"), lax.axis_index("xl")
    rows = pl.ds(pl.multiple_of(xl * 32, 32), 32)
    for half in range(2):
        mixed = parts_ref[half, 0].astype(F32)
        for k in range(1, 8):
            mixed += parts_ref[half, k].astype(F32)
        up = left_ref[half * 4 + zl * 2 + xh, 1, rows].astype(F32)
        update = (up / root_ref[pl.ds(half * 32, 32)] + factor * mixed).astype(BF16)
        for k in range(out_ref.shape[0]):
            out_ref[k, half] = update


def split_l_kernel(kept_ref, came_ref, keep_ref, send_ref):
    zl, xl = lax.axis_index("zl"), lax.axis_index("xl")
    for from_z, ref in ((zl, kept_ref), (zl ^ 1, came_ref)):
        for to_h in range(2):
            keep_ref[from_z, to_h] = ref[to_h * 2 + xl]
            send_ref[from_z, to_h] = ref[to_h * 2 + (xl ^ 1)]


def split_h_kernel(kept_ref, came_ref, keep_ref, send_ref):
    xh, xl = lax.axis_index("xh"), lax.axis_index("xl")
    for from_l, ref in ((xl, kept_ref), (xl ^ 1, came_ref)):
        for from_z in range(2):
            keep_ref[from_z, from_l] = ref[from_z, xh]
            send_ref[from_z, from_l] = ref[from_z, xh ^ 1]


def finish_kernel(kept_ref, came_ref, every_ref, out_ref, basis):
    xh = lax.axis_index("xh")
    tokens = every_ref.shape[3]
    for from_h, ref in ((xh, kept_ref), (xh ^ 1, came_ref)):
        for from_z in range(2):
            blocks = [ref[from_z, from_l, lb] for from_l in range(2) for lb in range(2)]
            basis[from_z * 2 + from_h] = jnp.concatenate(blocks, 1)
    rows = [
        every_ref[xl * 4 + r, half] for half in range(2) for r in range(4) for xl in range(2)
    ]
    part = jnp.dot(
        basis[...].reshape(512, 512), jnp.concatenate(rows, 0), preferred_element_type=F32
    )
    out_ref[...] = part.astype(BF16).reshape(-1, 64, tokens)


def on_device(inputs, upstream, eig_tiles, eigvals):
    zl, xh, xl, y = (lax.axis_index(a) for a in ("zl", "xh", "xl", "y"))
    zh, core = lax.axis_index("zh"), lax.axis_index("core")
    tokens = inputs.shape[0]
    eig = eig_tiles[0]
    r = zl * 2 + xh

    by_b = lax.dynamic_index_in_dim(eigvals.reshape(2, 2, 8, 128), y, 2, keepdims=False)
    lam_b = jnp.transpose(by_b, (1, 0, 2)).reshape(8, 64)
    cube = jnp.transpose(eigvals.reshape(2, 2, 8, 2, 64), (0, 3, 1, 2, 4)).reshape(8, 8, 64)
    lam_a = lax.dynamic_index_in_dim(cube, r * 2 + xl, 0, keepdims=False)
    by_half = lax.dynamic_index_in_dim(lam_b.reshape(2, 4, 2, 32), r, 1, keepdims=False)
    lam_own = lax.dynamic_index_in_dim(by_half, xl, 1, keepdims=False).reshape(64, 1)
    lam_rows = lax.dynamic_index_in_dim(lam_b, core * 4 + zh, 0, keepdims=False).reshape(64, 1)
    lam_cols = lam_a.reshape(1, 512)

    parts = project(inputs, upstream, eig)
    got = lax.all_to_all(parts, ROWS, 0, 0, tiled=True)
    own, copies = call(
        spread_kernel, (got,), (out(BF16, 2, 64, tokens), out(BF16, 8, 2, 64, tokens))
    )
    halves = eig.reshape(2, 4, 2, 128, 128)
    right = lax.all_to_all(copies, "y", 0, 0, tiled=True)
    away = lax.dynamic_index_in_dim(halves, 1 - zl, 0, keepdims=False)
    kept = lax.dynamic_index_in_dim(halves, zl, 0, keepdims=False)
    came = lax.ppermute(away, "zl", SWAP)
    quarter = out(BF16, 2, 2, 2, 128, 128)
    keep_l, send_l = call(split_l_kernel, (kept, came), (quarter, quarter))
    got_l = lax.ppermute(send_l, "xl", SWAP)
    s_rows, s_cols, s_own = call(
        roots_kernel,
        (lam_rows, lam_cols, lam_own),
        (out(F32, 64, 1), out(F32, 1, 512), out(F32, 64, 1)),
    )
    again = jnp.broadcast_to(own[None], (8, *own.shape))
    left = lax.all_to_all(again, COLS, 0, 0, tiled=True)

    half_block = out(BF16, 256, 512)
    send = call(gram_kernel(1), (left, right), half_block)
    other = lax.ppermute(send, "core", SWAP)
    keep = call(gram_kernel(0), (left, right), half_block)
    both = call(add_kernel, (keep, other), out(BF16, 4, 64, 512))

    shares = lax.all_to_all(both, "zh", 0, 0, tiled=True)
    keep_h, send_h = call(split_h_kernel, (keep_l, got_l), (quarter, quarter))
    got_h = lax.ppermute(send_h, "xh", SWAP)
    other_in = lax.ppermute(right[:, 0], "core", SWAP)
    part = call(weigh_kernel, (shares, s_rows, s_cols), out(BF16, 4, 64, 512))
    mine = lax.all_to_all(part, "zh", 0, 0, tiled=True)
    mixed_part = call(mix_kernel, (mine, right, other_in), out(BF16, 2, 2, 4, 32, tokens))
    mixed = lax.all_to_all(mixed_part.reshape(16, 32, tokens), ("core", *COLS), 0, 0, tiled=True)
    factor = 2.0 / (8 * tokens)
    update = call(
        lambda *refs: update_kernel(factor, *refs),
        (mixed.reshape(2, 8, 32, tokens), left, s_own),
        out(BF16, 8, 2, 32, tokens),
    )
    every = lax.all_to_all(update, COLS, 0, 0, tiled=True)
    grad_part = call(
        finish_kernel,
        (keep_h, got_h, every),
        out(BF16, 8, 64, tokens),
        (pltpu.VMEM((4, 128, 512), BF16),),
    )
    blocks = lax.all_to_all(grad_part, "y", 0, 0, tiled=True)
    return jnp.sum(blocks.astype(F32), 0).astype(BF16)


def solution(mesh):
    grid = Mesh(mesh.devices.reshape(SIZES), AXES)
    dp, mp = AXES[:2], AXES[2:]
    return jax.shard_map(
        on_device,
        mesh=grid,
        in_specs=(P(dp, None), P(dp, None), P(mp, None, None, None, None), P()),
        out_specs=P(mp, dp),
        check_vma=False,
    )
```

```python
import jax
import jax.numpy as jnp
from jax import lax
from jax.experimental import pallas as pl
from jax.experimental.pallas import tpu as pltpu
from jax.sharding import Mesh
from jax.sharding import PartitionSpec as P

F32 = jnp.float32
BF16 = jnp.bfloat16
AXES = ("zh", "core", "zl", "xh", "xl", "y")
SIZES = (4, 2, 2, 2, 2, 8)
ROWS = ("zl", "xh")
COLS = ("xl", "zl", "xh")
SWAP = [(0, 1), (1, 0)]

ANYWHERE = pl.BlockSpec(memory_space=pl.ANY)
IN_VMEM = pl.BlockSpec(memory_space=pltpu.VMEM)


def call(kernel, arrays, outs, scratch=()):
    held = [pltpu.with_memory_space_constraint(a, pltpu.VMEM) for a in arrays]
    single = not isinstance(outs, (list, tuple))
    shapes = [outs] if single else outs
    got = pl.pallas_call(
        kernel,
        out_shape=[pltpu.VMEM(s, d) for s, d in shapes_of(shapes)],
        in_specs=[IN_VMEM] * len(held),
        out_specs=[IN_VMEM] * len(shapes),
        scratch_shapes=list(scratch),
    )(*held)
    return got[0] if single else got


def shapes_of(outs):
    return [(o.shape, o.dtype) for o in outs]


def out(dtype, *shape):
    return jax.ShapeDtypeStruct(shape, dtype)


def project_kernel(x_ref, y_ref, eig_ref, out_ref, xs, tiles, sems, tile_sem):
    steps = eig_ref.shape[0]
    grid_rows = x_ref.shape[1] // (steps * 128)
    r = lax.axis_index("zl") * 2 + lax.axis_index("xh")

    def copy(s, la):
        src = x_ref if s == 0 else y_ref
        start = pl.multiple_of((la * grid_rows + r) * 128, 128)
        return pltpu.make_async_copy(
            src.at[:, pl.ds(start, 128)], xs.at[s, :, pl.ds(la * 128, 128)], sems.at[s, la]
        )

    load = pltpu.make_async_copy(eig_ref, tiles, tile_sem)
    load.start()
    for s in range(2):
        for la in range(steps):
            copy(s, la).start()
    load.wait()
    basis = jnp.concatenate(
        [tiles[:, lb].reshape(steps * 128, 128) for lb in range(tiles.shape[1])], 1
    )
    for s in range(2):
        for la in range(steps):
            copy(s, la).wait()
        part = jnp.dot(xs[s], basis, preferred_element_type=F32)
        turned = part.T.astype(BF16)
        out_ref[:, s] = turned.reshape(out_ref.shape[0], *out_ref.shape[2:])


def project(inputs, upstream, eig):
    tokens = inputs.shape[0]
    steps = eig.shape[0]
    return pl.pallas_call(
        project_kernel,
        out_shape=pltpu.VMEM((4, 2, 64, tokens), BF16),
        in_specs=[ANYWHERE] * 3,
        out_specs=IN_VMEM,
        scratch_shapes=[
            pltpu.VMEM((2, tokens, steps * 128), BF16),
            pltpu.VMEM(eig.shape, BF16),
            pltpu.SemaphoreType.DMA((2, steps)),
            pltpu.SemaphoreType.DMA,
        ],
        name="project",
    )(inputs, upstream, eig)


def spread_kernel(parts_ref, own_ref, copies_ref):
    total = parts_ref[0].astype(F32)
    for k in range(1, parts_ref.shape[0]):
        total += parts_ref[k].astype(F32)
    own = total.astype(BF16)
    own_ref[...] = own
    for k in range(copies_ref.shape[0]):
        copies_ref[k] = own


def again_kernel(own_ref, out_ref):
    for core in range(2):
        for k in range(8):
            out_ref[core * 8 + k] = own_ref[:, core * 32 : core * 32 + 32]


def gram_kernel(b_ref, a_ref, other_ref, out_ref):
    core = lax.axis_index("core")
    tokens = a_ref.shape[3]
    block = jnp.zeros(out_ref.shape, F32).reshape(256, -1)
    for of, ref in ((core, a_ref), (core ^ 1, other_ref)):
        for s in range(2):
            block += lax.dot_general(
                b_ref[of, :, s].reshape(256, tokens),
                ref[:, 1 - s].reshape(-1, tokens),
                (((1,), (1,)), ((), ())),
                preferred_element_type=F32,
            )
    out_ref[...] = block.astype(BF16).reshape(out_ref.shape)


def roots_kernel(*refs):
    for k in range(3):
        refs[3 + k][...] = jnp.sqrt(refs[k][...])


def weigh_kernel(parts_ref, rows_ref, cols_ref, out_ref):
    share = parts_ref[0].astype(F32)
    for k in range(1, parts_ref.shape[0]):
        share += parts_ref[k].astype(F32)
    s_b, s_a = rows_ref[...], cols_ref[...]
    kernel = -1.0 / (s_b * s_a * (s_b + s_a))
    part = (kernel * (0.5 * share)).astype(BF16)
    for k in range(out_ref.shape[0]):
        out_ref[k] = part


def mix_kernel(half_ref, a_ref, other_ref, out_ref):
    core = lax.axis_index("core")
    tokens = a_ref.shape[3]
    weights = half_ref[...].reshape(256, -1)
    for to, ref in ((core, a_ref), (core ^ 1, other_ref)):
        proj_in = ref[:, 0].reshape(-1, tokens)
        part = jnp.dot(weights, proj_in, preferred_element_type=F32)
        out_ref[to] = part.astype(BF16).reshape(8, 32, tokens)


def update_kernel(factor, parts_ref, own_ref, root_ref, out_ref):
    for half in range(2):
        mixed = parts_ref[half, 0].astype(F32)
        for k in range(1, 8):
            mixed += parts_ref[half, k].astype(F32)
        rows = pl.ds(half * 32, 32)
        update = own_ref[1, rows].astype(F32) / root_ref[rows] + factor * mixed
        update = update.astype(BF16)
        for k in range(out_ref.shape[0]):
            out_ref[k, rows] = update


def split_l_kernel(kept_ref, came_ref, keep_ref, send_ref):
    zl, xl = lax.axis_index("zl"), lax.axis_index("xl")
    for from_z, ref in ((zl, kept_ref), (zl ^ 1, came_ref)):
        for to_h in range(2):
            keep_ref[from_z, to_h] = ref[to_h * 2 + xl]
            send_ref[from_z, to_h] = ref[to_h * 2 + (xl ^ 1)]


def split_h_kernel(kept_ref, came_ref, keep_ref, send_ref):
    xh, xl = lax.axis_index("xh"), lax.axis_index("xl")
    for from_l, ref in ((xl, kept_ref), (xl ^ 1, came_ref)):
        for from_z in range(2):
            keep_ref[from_z, from_l] = ref[from_z, xh]
            send_ref[from_z, from_l] = ref[from_z, xh ^ 1]


def finish_kernel(kept_ref, came_ref, every_ref, out_ref, basis):
    xh = lax.axis_index("xh")
    tokens = every_ref.shape[2]
    for from_h, ref in ((xh, kept_ref), (xh ^ 1, came_ref)):
        for from_z in range(2):
            blocks = [ref[from_z, from_l, lb] for from_l in range(2) for lb in range(2)]
            basis[from_z * 2 + from_h] = jnp.concatenate(blocks, 1)
    part = jnp.dot(
        basis[...].reshape(512, 512),
        every_ref[...].reshape(512, tokens),
        preferred_element_type=F32,
    )
    out_ref[...] = part.astype(BF16).reshape(-1, 64, tokens)


def on_device(inputs, upstream, eig_tiles, eigvals):
    zl, xh, xl, y = (lax.axis_index(a) for a in ("zl", "xh", "xl", "y"))
    zh, core = lax.axis_index("zh"), lax.axis_index("core")
    tokens = inputs.shape[0]
    eig = eig_tiles[0]
    r = zl * 2 + xh

    by_b = lax.dynamic_index_in_dim(eigvals.reshape(2, 2, 8, 128), y, 2, keepdims=False)
    lam_b = jnp.transpose(by_b, (1, 0, 2)).reshape(8, 64)
    cube = jnp.transpose(eigvals.reshape(2, 2, 8, 2, 64), (0, 3, 1, 2, 4)).reshape(8, 8, 64)
    lam_a = lax.dynamic_index_in_dim(cube, r * 2 + xl, 0, keepdims=False)
    lam_own = lax.dynamic_index_in_dim(lam_a, y, 0, keepdims=False).reshape(64, 1)
    by_core = lax.dynamic_index_in_dim(lam_b.reshape(4, 2, 2, 32), core, 2, keepdims=False)
    lam_rows = lax.dynamic_index_in_dim(by_core, zh, 0, keepdims=False).reshape(64, 1)
    lam_cols = lam_a.reshape(1, 512)

    parts = project(inputs, upstream, eig)
    got = lax.all_to_all(parts, ROWS, 0, 0, tiled=True)
    own, copies = call(
        spread_kernel, (got,), (out(BF16, 2, 64, tokens), out(BF16, 8, 2, 64, tokens))
    )
    halves = eig.reshape(2, 4, 2, 128, 128)
    right = lax.all_to_all(copies, "y", 0, 0, tiled=True)
    away = lax.dynamic_index_in_dim(halves, 1 - zl, 0, keepdims=False)
    kept = lax.dynamic_index_in_dim(halves, zl, 0, keepdims=False)
    came = lax.ppermute(away, "zl", SWAP)
    quarter = out(BF16, 2, 2, 2, 128, 128)
    keep_l, send_l = call(split_l_kernel, (kept, came), (quarter, quarter))
    got_l = lax.ppermute(send_l, "xl", SWAP)
    s_rows, s_cols, s_own = call(
        roots_kernel,
        (lam_rows, lam_cols, lam_own),
        (out(F32, 64, 1), out(F32, 1, 512), out(F32, 64, 1)),
    )
    again = call(again_kernel, (own,), out(BF16, 16, 2, 32, tokens))
    left = lax.all_to_all(again, ("core", *COLS), 0, 0, tiled=True)
    other = lax.ppermute(right, "core", SWAP)
    both = call(
        gram_kernel, (left.reshape(2, 8, 2, 32, tokens), right, other), out(BF16, 4, 64, 512)
    )

    shares = lax.all_to_all(both, "zh", 0, 0, tiled=True)
    keep_h, send_h = call(split_h_kernel, (keep_l, got_l), (quarter, quarter))
    got_h = lax.ppermute(send_h, "xh", SWAP)
    part = call(weigh_kernel, (shares, s_rows, s_cols), out(BF16, 4, 64, 512))
    mine = lax.all_to_all(part, "zh", 0, 0, tiled=True)
    mixed_part = call(mix_kernel, (mine, right, other), out(BF16, 2, 8, 32, tokens))
    mixed = lax.all_to_all(mixed_part.reshape(16, 32, tokens), ("core", *COLS), 0, 0, tiled=True)
    factor = 2.0 / (8 * tokens)
    update = call(
        lambda *refs: update_kernel(factor, *refs),
        (mixed.reshape(2, 8, 32, tokens), own, s_own),
        out(BF16, 8, 64, tokens),
    )
    every = lax.all_to_all(update, COLS, 0, 0, tiled=True)
    grad_part = call(
        finish_kernel,
        (keep_h, got_h, every),
        out(BF16, 8, 64, tokens),
        (pltpu.VMEM((4, 128, 512), BF16),),
    )
    blocks = lax.all_to_all(grad_part, "y", 0, 0, tiled=True)
    return jnp.sum(blocks.astype(F32), 0).astype(BF16)


def solution(mesh):
    grid = Mesh(mesh.devices.reshape(SIZES), AXES)
    dp, mp = AXES[:2], AXES[2:]
    return jax.shard_map(
        on_device,
        mesh=grid,
        in_specs=(P(dp, None), P(dp, None), P(mp, None, None, None, None), P()),
        out_specs=P(mp, dp),
        check_vma=False,
    )
```

```python
import jax
import jax.numpy as jnp
from jax import lax
from jax.experimental import pallas as pl
from jax.experimental.pallas import tpu as pltpu
from jax.sharding import Mesh
from jax.sharding import PartitionSpec as P

F32 = jnp.float32
BF16 = jnp.bfloat16
AXES = ("zh", "core", "zl", "xh", "xl", "y")
SIZES = (4, 2, 2, 2, 2, 8)
ROWS = ("zl", "xh")
COLS = ("xl", "zl", "xh")
SWAP = [(0, 1), (1, 0)]

ANYWHERE = pl.BlockSpec(memory_space=pl.ANY)
IN_VMEM = pl.BlockSpec(memory_space=pltpu.VMEM)


def call(kernel, arrays, outs, scratch=()):
    held = [pltpu.with_memory_space_constraint(a, pltpu.VMEM) for a in arrays]
    single = not isinstance(outs, (list, tuple))
    shapes = [outs] if single else outs
    got = pl.pallas_call(
        kernel,
        out_shape=[pltpu.VMEM(s, d) for s, d in shapes_of(shapes)],
        in_specs=[IN_VMEM] * len(held),
        out_specs=[IN_VMEM] * len(shapes),
        scratch_shapes=list(scratch),
    )(*held)
    return got[0] if single else got


def shapes_of(outs):
    return [(o.shape, o.dtype) for o in outs]


def out(dtype, *shape):
    return jax.ShapeDtypeStruct(shape, dtype)


def project_kernel(x_ref, y_ref, eig_ref, out_ref, xs, tiles, sems, tile_sem):
    steps = eig_ref.shape[0]
    grid_rows = x_ref.shape[1] // (steps * 128)
    r = lax.axis_index("zl") * 2 + lax.axis_index("xh")

    def copy(s, la):
        src = x_ref if s == 0 else y_ref
        start = pl.multiple_of((la * grid_rows + r) * 128, 128)
        return pltpu.make_async_copy(
            src.at[:, pl.ds(start, 128)], xs.at[s, :, pl.ds(la * 128, 128)], sems.at[s, la]
        )

    load = pltpu.make_async_copy(eig_ref, tiles, tile_sem)
    load.start()
    for s in range(2):
        for la in range(steps):
            copy(s, la).start()
    load.wait()
    basis = jnp.concatenate(
        [tiles[:, lb].reshape(steps * 128, 128) for lb in range(tiles.shape[1])], 1
    )
    for s in range(2):
        for la in range(steps):
            copy(s, la).wait()
        part = jnp.dot(xs[s], basis, preferred_element_type=F32)
        turned = part.T.astype(BF16)
        out_ref[:, s] = turned.reshape(out_ref.shape[0], *out_ref.shape[2:])


def project(inputs, upstream, eig):
    tokens = inputs.shape[0]
    steps = eig.shape[0]
    return pl.pallas_call(
        project_kernel,
        out_shape=pltpu.VMEM((4, 2, 64, tokens), BF16),
        in_specs=[ANYWHERE] * 3,
        out_specs=IN_VMEM,
        scratch_shapes=[
            pltpu.VMEM((2, tokens, steps * 128), BF16),
            pltpu.VMEM(eig.shape, BF16),
            pltpu.SemaphoreType.DMA((2, steps)),
            pltpu.SemaphoreType.DMA,
        ],
        name="project",
    )(inputs, upstream, eig)


def spread_kernel(parts_ref, own_ref, halves_ref, copies_ref):
    total = parts_ref[0].astype(F32)
    for k in range(1, parts_ref.shape[0]):
        total += parts_ref[k].astype(F32)
    own = total.astype(BF16)
    own_ref[...] = own
    for k in range(copies_ref.shape[0]):
        copies_ref[k] = own
    for core in range(2):
        for k in range(8):
            halves_ref[core * 8 + k] = own[:, core * 32 : core * 32 + 32]


def gram_own_kernel(b_ref, a_ref, out_ref):
    tokens = a_ref.shape[3]
    core = lax.axis_index("core")
    out_ref[...] = gram_part(b_ref, core, a_ref, tokens)


def gram_other_kernel(b_ref, a_ref, first_ref, out_ref):
    tokens = a_ref.shape[3]
    core = lax.axis_index("core")
    block = first_ref[...] + gram_part(b_ref, core ^ 1, a_ref, tokens)
    out_ref[...] = block.astype(BF16).reshape(out_ref.shape)


def gram_part(b_ref, of, a_ref, tokens):
    over = (((1,), (1,)), ((), ()))
    part = [
        lax.dot_general(
            b_ref[of, :, s].reshape(256, tokens),
            a_ref[:, 1 - s].reshape(-1, tokens),
            over,
            preferred_element_type=F32,
        )
        for s in range(2)
    ]
    return part[0] + part[1]


def roots_kernel(*refs):
    for k in range(3):
        refs[3 + k][...] = jnp.sqrt(refs[k][...])


def weigh_kernel(parts_ref, rows_ref, cols_ref, out_ref):
    share = parts_ref[0].astype(F32)
    for k in range(1, parts_ref.shape[0]):
        share += parts_ref[k].astype(F32)
    s_b, s_a = rows_ref[...], cols_ref[...]
    kernel = -1.0 / (s_b * s_a * (s_b + s_a))
    part = (kernel * (0.5 * share)).astype(BF16)
    for k in range(out_ref.shape[0]):
        out_ref[k] = part


def mix_kernel(half_ref, a_ref, other_ref, out_ref):
    core = lax.axis_index("core")
    tokens = a_ref.shape[3]
    weights = half_ref[...].reshape(256, -1)
    for to, ref in ((core, a_ref), (core ^ 1, other_ref)):
        proj_in = ref[:, 0].reshape(-1, tokens)
        part = jnp.dot(weights, proj_in, preferred_element_type=F32)
        out_ref[to] = part.astype(BF16).reshape(8, 32, tokens)


def update_kernel(factor, parts_ref, own_ref, root_ref, out_ref):
    for half in range(2):
        mixed = parts_ref[half, 0].astype(F32)
        for k in range(1, 8):
            mixed += parts_ref[half, k].astype(F32)
        rows = pl.ds(half * 32, 32)
        update = own_ref[1, rows].astype(F32) / root_ref[rows] + factor * mixed
        update = update.astype(BF16)
        for k in range(out_ref.shape[0]):
            out_ref[k, rows] = update


def split_l_kernel(kept_ref, came_ref, keep_ref, send_ref):
    zl, xl = lax.axis_index("zl"), lax.axis_index("xl")
    for from_z, ref in ((zl, kept_ref), (zl ^ 1, came_ref)):
        for to_h in range(2):
            keep_ref[from_z, to_h] = ref[to_h * 2 + xl]
            send_ref[from_z, to_h] = ref[to_h * 2 + (xl ^ 1)]


def split_h_kernel(kept_ref, came_ref, keep_ref, send_ref):
    xh, xl = lax.axis_index("xh"), lax.axis_index("xl")
    for from_l, ref in ((xl, kept_ref), (xl ^ 1, came_ref)):
        for from_z in range(2):
            keep_ref[from_z, from_l] = ref[from_z, xh]
            send_ref[from_z, from_l] = ref[from_z, xh ^ 1]


def finish_kernel(kept_ref, came_ref, every_ref, out_ref, basis):
    xh = lax.axis_index("xh")
    tokens = every_ref.shape[2]
    for from_h, ref in ((xh, kept_ref), (xh ^ 1, came_ref)):
        for from_z in range(2):
            blocks = [ref[from_z, from_l, lb] for from_l in range(2) for lb in range(2)]
            basis[from_z * 2 + from_h] = jnp.concatenate(blocks, 1)
    part = jnp.dot(
        basis[...].reshape(512, 512),
        every_ref[...].reshape(512, tokens),
        preferred_element_type=F32,
    )
    out_ref[...] = part.astype(BF16).reshape(-1, 64, tokens)


def on_device(inputs, upstream, eig_tiles, eigvals):
    zl, xh, xl, y = (lax.axis_index(a) for a in ("zl", "xh", "xl", "y"))
    zh, core = lax.axis_index("zh"), lax.axis_index("core")
    tokens = inputs.shape[0]
    eig = eig_tiles[0]
    r = zl * 2 + xh

    by_b = lax.dynamic_index_in_dim(eigvals.reshape(2, 2, 8, 128), y, 2, keepdims=False)
    lam_b = jnp.transpose(by_b, (1, 0, 2)).reshape(8, 64)
    cube = jnp.transpose(eigvals.reshape(2, 2, 8, 2, 64), (0, 3, 1, 2, 4)).reshape(8, 8, 64)
    lam_a = lax.dynamic_index_in_dim(cube, r * 2 + xl, 0, keepdims=False)
    lam_own = lax.dynamic_index_in_dim(lam_a, y, 0, keepdims=False).reshape(64, 1)
    by_core = lax.dynamic_index_in_dim(lam_b.reshape(4, 2, 2, 32), core, 2, keepdims=False)
    lam_rows = lax.dynamic_index_in_dim(by_core, zh, 0, keepdims=False).reshape(64, 1)
    lam_cols = lam_a.reshape(1, 512)

    parts = project(inputs, upstream, eig)
    got = lax.all_to_all(parts, ROWS, 0, 0, tiled=True)
    own, pieces, copies = call(
        spread_kernel,
        (got,),
        (
            out(BF16, 2, 64, tokens),
            out(BF16, 16, 2, 32, tokens),
            out(BF16, 8, 2, 64, tokens),
        ),
    )
    left = lax.all_to_all(pieces, ("core", *COLS), 0, 0, tiled=True)
    left = left.reshape(2, 8, 2, 32, tokens)
    halves = eig.reshape(2, 4, 2, 128, 128)
    right = lax.all_to_all(copies, "y", 0, 0, tiled=True)
    away = lax.dynamic_index_in_dim(halves, 1 - zl, 0, keepdims=False)
    kept = lax.dynamic_index_in_dim(halves, zl, 0, keepdims=False)
    came = lax.ppermute(away, "zl", SWAP)
    quarter = out(BF16, 2, 2, 2, 128, 128)
    keep_l, send_l = call(split_l_kernel, (kept, came), (quarter, quarter))
    got_l = lax.ppermute(send_l, "xl", SWAP)
    s_rows, s_cols, s_own = call(
        roots_kernel,
        (lam_rows, lam_cols, lam_own),
        (out(F32, 64, 1), out(F32, 1, 512), out(F32, 64, 1)),
    )
    other = lax.ppermute(right, "core", SWAP)
    first = call(gram_own_kernel, (left, right), out(F32, 256, 512))
    both = call(gram_other_kernel, (left, other, first), out(BF16, 4, 64, 512))

    shares = lax.all_to_all(both, "zh", 0, 0, tiled=True)
    keep_h, send_h = call(split_h_kernel, (keep_l, got_l), (quarter, quarter))
    got_h = lax.ppermute(send_h, "xh", SWAP)
    part = call(weigh_kernel, (shares, s_rows, s_cols), out(BF16, 4, 64, 512))
    mine = lax.all_to_all(part, "zh", 0, 0, tiled=True)
    mixed_part = call(mix_kernel, (mine, right, other), out(BF16, 2, 8, 32, tokens))
    mixed = lax.all_to_all(mixed_part.reshape(16, 32, tokens), ("core", *COLS), 0, 0, tiled=True)
    factor = 2.0 / (8 * tokens)
    update = call(
        lambda *refs: update_kernel(factor, *refs),
        (mixed.reshape(2, 8, 32, tokens), own, s_own),
        out(BF16, 8, 64, tokens),
    )
    every = lax.all_to_all(update, COLS, 0, 0, tiled=True)
    grad_part = call(
        finish_kernel,
        (keep_h, got_h, every),
        out(BF16, 8, 64, tokens),
        (pltpu.VMEM((4, 128, 512), BF16),),
    )
    blocks = lax.all_to_all(grad_part, "y", 0, 0, tiled=True)
    return jnp.sum(blocks.astype(F32), 0).astype(BF16)


def solution(mesh):
    grid = Mesh(mesh.devices.reshape(SIZES), AXES)
    dp, mp = AXES[:2], AXES[2:]
    return jax.shard_map(
        on_device,
        mesh=grid,
        in_specs=(P(dp, None), P(dp, None), P(mp, None, None, None, None), P()),
        out_specs=P(mp, dp),
        check_vma=False,
    )
```

```python
import jax
import jax.numpy as jnp
from jax import lax
from jax.experimental import pallas as pl
from jax.experimental.pallas import tpu as pltpu
from jax.sharding import Mesh
from jax.sharding import PartitionSpec as P

F32 = jnp.float32
BF16 = jnp.bfloat16
AXES = ("zh1", "zh0", "core", "zl", "xh", "xl", "y2", "y1", "y0")
SIZES = (2,) * 9
ROWS = ("xh", "zl")
LINE = ("y0", "y1", "y2")
DEPTH = ("zh0", "zh1")
COLS = ("xl", "zl", "xh")
SWAP = [(0, 1), (1, 0)]

ANYWHERE = pl.BlockSpec(memory_space=pl.ANY)
IN_VMEM = pl.BlockSpec(memory_space=pltpu.VMEM)


def call(kernel, arrays, outs, scratch=()):
    held = [pltpu.with_memory_space_constraint(a, pltpu.VMEM) for a in arrays]
    single = not isinstance(outs, (list, tuple))
    shapes = [outs] if single else outs
    got = pl.pallas_call(
        kernel,
        out_shape=[pltpu.VMEM(s, d) for s, d in shapes_of(shapes)],
        in_specs=[IN_VMEM] * len(held),
        out_specs=[IN_VMEM] * len(shapes),
        scratch_shapes=list(scratch),
    )(*held)
    return got[0] if single else got


def shapes_of(outs):
    return [(o.shape, o.dtype) for o in outs]


def out(dtype, *shape):
    return jax.ShapeDtypeStruct(shape, dtype)


def project_kernel(x_ref, y_ref, eig_ref, out_ref, xs, tiles, sems, tile_sem):
    steps = eig_ref.shape[0]
    grid_rows = x_ref.shape[1] // (steps * 128)
    r = lax.axis_index("zl") * 2 + lax.axis_index("xh")

    def copy(s, la):
        src = x_ref if s == 0 else y_ref
        start = pl.multiple_of((la * grid_rows + r) * 128, 128)
        return pltpu.make_async_copy(
            src.at[:, pl.ds(start, 128)], xs.at[s, :, pl.ds(la * 128, 128)], sems.at[s, la]
        )

    load = pltpu.make_async_copy(eig_ref, tiles, tile_sem)
    load.start()
    for s in range(2):
        for la in range(steps):
            copy(s, la).start()
    load.wait()
    basis = jnp.concatenate(
        [tiles[:, lb].reshape(steps * 128, 128) for lb in range(tiles.shape[1])], 1
    )
    for s in range(2):
        for la in range(steps):
            copy(s, la).wait()
        part = jnp.dot(xs[s], basis, preferred_element_type=F32)
        turned = part.T.astype(BF16)
        turned = turned.reshape(out_ref.shape[0], *out_ref.shape[2:])
        for zl in range(2):
            for xh in range(2):
                out_ref[xh * 2 + zl, s] = turned[zl * 2 + xh]


def project(inputs, upstream, eig):
    tokens = inputs.shape[0]
    steps = eig.shape[0]
    return pl.pallas_call(
        project_kernel,
        out_shape=pltpu.VMEM((4, 2, 64, tokens), BF16),
        in_specs=[ANYWHERE] * 3,
        out_specs=IN_VMEM,
        scratch_shapes=[
            pltpu.VMEM((2, tokens, steps * 128), BF16),
            pltpu.VMEM(eig.shape, BF16),
            pltpu.SemaphoreType.DMA((2, steps)),
            pltpu.SemaphoreType.DMA,
        ],
        name="project",
    )(inputs, upstream, eig)


def spread_kernel(parts_ref, own_ref, copies_ref):
    total = parts_ref[0].astype(F32)
    for k in range(1, parts_ref.shape[0]):
        total += parts_ref[k].astype(F32)
    own = total.astype(BF16)
    own_ref[...] = own
    for k in range(copies_ref.shape[0]):
        copies_ref[k] = own


def again_kernel(own_ref, out_ref):
    for core in range(2):
        for k in range(8):
            out_ref[core * 8 + k] = own_ref[:, core * 32 : core * 32 + 32]


def gram_kernel(b_ref, a_ref, other_ref, out_ref):
    core = lax.axis_index("core")
    tokens = a_ref.shape[3]
    block = jnp.zeros(out_ref.shape, F32).reshape(256, -1)
    for of, ref in ((core, a_ref), (core ^ 1, other_ref)):
        for s in range(2):
            block += lax.dot_general(
                b_ref[of, :, s].reshape(256, tokens),
                ref[:, 1 - s].reshape(-1, tokens),
                (((1,), (1,)), ((), ())),
                preferred_element_type=F32,
            )
    out_ref[...] = block.astype(BF16).reshape(out_ref.shape)


def roots_kernel(*refs):
    for k in range(3):
        refs[3 + k][...] = jnp.sqrt(refs[k][...])


def weigh_kernel(parts_ref, rows_ref, cols_ref, out_ref):
    share = parts_ref[0].astype(F32)
    for k in range(1, parts_ref.shape[0]):
        share += parts_ref[k].astype(F32)
    s_b, s_a = rows_ref[...], cols_ref[...]
    kernel = -1.0 / (s_b * s_a * (s_b + s_a))
    part = (kernel * (0.5 * share)).astype(BF16)
    for k in range(out_ref.shape[0]):
        out_ref[k] = part


def mix_kernel(half_ref, a_ref, other_ref, out_ref):
    core = lax.axis_index("core")
    tokens = a_ref.shape[3]
    weights = half_ref[...].reshape(256, -1)
    for to, ref in ((core, a_ref), (core ^ 1, other_ref)):
        proj_in = ref[:, 0].reshape(-1, tokens)
        part = jnp.dot(weights, proj_in, preferred_element_type=F32)
        out_ref[to] = part.astype(BF16).reshape(8, 32, tokens)


def update_kernel(factor, parts_ref, own_ref, root_ref, out_ref):
    for half in range(2):
        mixed = parts_ref[half, 0].astype(F32)
        for k in range(1, 8):
            mixed += parts_ref[half, k].astype(F32)
        rows = pl.ds(half * 32, 32)
        update = own_ref[1, rows].astype(F32) / root_ref[rows] + factor * mixed
        update = update.astype(BF16)
        for k in range(out_ref.shape[0]):
            out_ref[k, rows] = update


def split_l_kernel(kept_ref, came_ref, keep_ref, send_ref):
    zl, xl = lax.axis_index("zl"), lax.axis_index("xl")
    for from_z, ref in ((zl, kept_ref), (zl ^ 1, came_ref)):
        for to_h in range(2):
            keep_ref[from_z, to_h] = ref[to_h * 2 + xl]
            send_ref[from_z, to_h] = ref[to_h * 2 + (xl ^ 1)]


def split_h_kernel(kept_ref, came_ref, keep_ref, send_ref):
    xh, xl = lax.axis_index("xh"), lax.axis_index("xl")
    for from_l, ref in ((xl, kept_ref), (xl ^ 1, came_ref)):
        for from_z in range(2):
            keep_ref[from_z, from_l] = ref[from_z, xh]
            send_ref[from_z, from_l] = ref[from_z, xh ^ 1]


def finish_kernel(kept_ref, came_ref, every_ref, out_ref, basis):
    xh = lax.axis_index("xh")
    tokens = every_ref.shape[2]
    for from_h, ref in ((xh, kept_ref), (xh ^ 1, came_ref)):
        for from_z in range(2):
            blocks = [ref[from_z, from_l, lb] for from_l in range(2) for lb in range(2)]
            basis[from_z * 2 + from_h] = jnp.concatenate(blocks, 1)
    part = jnp.dot(
        basis[...].reshape(512, 512),
        every_ref[...].reshape(512, tokens),
        preferred_element_type=F32,
    )
    part = part.astype(BF16).reshape(8, 64, tokens)
    for y in range(8):
        out_ref[(y & 1) * 4 + (y & 2) + (y >> 2)] = part[y]


def on_device(inputs, upstream, eig_tiles, eigvals):
    zl, xh, xl, core = (lax.axis_index(a) for a in ("zl", "xh", "xl", "core"))
    y = lax.axis_index(("y2", "y1", "y0"))
    share = lax.axis_index(DEPTH)
    tokens = inputs.shape[0]
    eig = eig_tiles[0]
    r = zl * 2 + xh

    by_b = lax.dynamic_index_in_dim(eigvals.reshape(2, 2, 8, 128), y, 2, keepdims=False)
    lam_b = jnp.transpose(by_b, (1, 0, 2)).reshape(8, 64)
    cube = jnp.transpose(eigvals.reshape(2, 2, 8, 2, 64), (0, 3, 1, 2, 4)).reshape(8, 8, 64)
    lam_a = lax.dynamic_index_in_dim(cube, r * 2 + xl, 0, keepdims=False)
    lam_own = lax.dynamic_index_in_dim(lam_a, y, 0, keepdims=False).reshape(64, 1)
    by_core = lax.dynamic_index_in_dim(lam_b.reshape(4, 2, 2, 32), core, 2, keepdims=False)
    lam_rows = lax.dynamic_index_in_dim(by_core, share, 0, keepdims=False).reshape(64, 1)
    lam_cols = jnp.transpose(lam_a.reshape(2, 2, 2, 64), (2, 1, 0, 3)).reshape(1, 512)

    parts = project(inputs, upstream, eig)
    got = lax.all_to_all(parts, ROWS, 0, 0, tiled=True)
    own, copies = call(
        spread_kernel, (got,), (out(BF16, 2, 64, tokens), out(BF16, 8, 2, 64, tokens))
    )
    halves = eig.reshape(2, 4, 2, 128, 128)
    right = lax.all_to_all(copies, LINE, 0, 0, tiled=True)
    away = lax.dynamic_index_in_dim(halves, 1 - zl, 0, keepdims=False)
    kept = lax.dynamic_index_in_dim(halves, zl, 0, keepdims=False)
    came = lax.ppermute(away, "zl", SWAP)
    quarter = out(BF16, 2, 2, 2, 128, 128)
    keep_l, send_l = call(split_l_kernel, (kept, came), (quarter, quarter))
    got_l = lax.ppermute(send_l, "xl", SWAP)
    s_rows, s_cols, s_own = call(
        roots_kernel,
        (lam_rows, lam_cols, lam_own),
        (out(F32, 64, 1), out(F32, 1, 512), out(F32, 64, 1)),
    )
    again = call(again_kernel, (own,), out(BF16, 16, 2, 32, tokens))
    left = lax.all_to_all(again, ("core", *COLS), 0, 0, tiled=True)
    other = lax.ppermute(right, "core", SWAP)
    both = call(
        gram_kernel, (left.reshape(2, 8, 2, 32, tokens), right, other), out(BF16, 4, 64, 512)
    )

    shares = lax.all_to_all(both, DEPTH, 0, 0, tiled=True)
    keep_h, send_h = call(split_h_kernel, (keep_l, got_l), (quarter, quarter))
    got_h = lax.ppermute(send_h, "xh", SWAP)
    part = call(weigh_kernel, (shares, s_rows, s_cols), out(BF16, 4, 64, 512))
    mine = lax.all_to_all(part, DEPTH, 0, 0, tiled=True)
    mixed_part = call(mix_kernel, (mine, right, other), out(BF16, 2, 8, 32, tokens))
    mixed = lax.all_to_all(mixed_part.reshape(16, 32, tokens), ("core", *COLS), 0, 0, tiled=True)
    factor = 2.0 / (8 * tokens)
    update = call(
        lambda *refs: update_kernel(factor, *refs),
        (mixed.reshape(2, 8, 32, tokens), own, s_own),
        out(BF16, 8, 64, tokens),
    )
    every = lax.all_to_all(update, COLS, 0, 0, tiled=True)
    grad_part = call(
        finish_kernel,
        (keep_h, got_h, every),
        out(BF16, 8, 64, tokens),
        (pltpu.VMEM((4, 128, 512), BF16),),
    )
    blocks = lax.all_to_all(grad_part, LINE, 0, 0, tiled=True)
    return jnp.sum(blocks.astype(F32), 0).astype(BF16)


def solution(mesh):
    grid = Mesh(mesh.devices.reshape(SIZES), AXES)
    dp, mp = AXES[:3], AXES[3:]
    return jax.shard_map(
        on_device,
        mesh=grid,
        in_specs=(P(dp, None), P(dp, None), P(mp, None, None, None, None), P()),
        out_specs=P(mp, dp),
        check_vma=False,
    )
```

```python
import jax
import jax.numpy as jnp
from jax import lax
from jax.experimental import pallas as pl
from jax.experimental.pallas import tpu as pltpu
from jax.sharding import Mesh
from jax.sharding import PartitionSpec as P

F32 = jnp.float32
BF16 = jnp.bfloat16
AXES = ("zh1", "zh0", "core", "zl", "xh", "xl", "y2", "y1", "y0")
SIZES = (2,) * 9
ROWS = ("xh", "zl")
LINE = ("y0", "y1", "y2")
DEPTH = ("zh0", "zh1")
COLS = ("xl", "zl", "xh")
CHIPS = ("core", "xh", "xl", "zl")
SWAP = [(0, 1), (1, 0)]

ANYWHERE = pl.BlockSpec(memory_space=pl.ANY)
IN_VMEM = pl.BlockSpec(memory_space=pltpu.VMEM)


def call(kernel, arrays, outs, scratch=()):
    held = [pltpu.with_memory_space_constraint(a, pltpu.VMEM) for a in arrays]
    single = not isinstance(outs, (list, tuple))
    shapes = [outs] if single else outs
    got = pl.pallas_call(
        kernel,
        out_shape=[pltpu.VMEM(s, d) for s, d in shapes_of(shapes)],
        in_specs=[IN_VMEM] * len(held),
        out_specs=[IN_VMEM] * len(shapes),
        scratch_shapes=list(scratch),
    )(*held)
    return got[0] if single else got


def shapes_of(outs):
    return [(o.shape, o.dtype) for o in outs]


def out(dtype, *shape):
    return jax.ShapeDtypeStruct(shape, dtype)


def project_kernel(x_ref, y_ref, eig_ref, out_ref, xs, tiles, sems, tile_sem):
    steps = eig_ref.shape[0]
    grid_rows = x_ref.shape[1] // (steps * 128)
    r = lax.axis_index("zl") * 2 + lax.axis_index("xh")

    def copy(s, la):
        src = x_ref if s == 0 else y_ref
        start = pl.multiple_of((la * grid_rows + r) * 128, 128)
        return pltpu.make_async_copy(
            src.at[:, pl.ds(start, 128)], xs.at[s, :, pl.ds(la * 128, 128)], sems.at[s, la]
        )

    load = pltpu.make_async_copy(eig_ref, tiles, tile_sem)
    load.start()
    for s in range(2):
        for la in range(steps):
            copy(s, la).start()
    load.wait()
    basis = jnp.concatenate(
        [tiles[:, lb].reshape(steps * 128, 128) for lb in range(tiles.shape[1])], 1
    )
    for s in range(2):
        for la in range(steps):
            copy(s, la).wait()
        part = jnp.dot(xs[s], basis, preferred_element_type=F32)
        turned = part.T.astype(BF16)
        turned = turned.reshape(out_ref.shape[0], *out_ref.shape[2:])
        for zl in range(2):
            for xh in range(2):
                out_ref[xh * 2 + zl, s] = turned[zl * 2 + xh]


def project(inputs, upstream, eig):
    tokens = inputs.shape[0]
    steps = eig.shape[0]
    return pl.pallas_call(
        project_kernel,
        out_shape=pltpu.VMEM((4, 2, 64, tokens), BF16),
        in_specs=[ANYWHERE] * 3,
        out_specs=IN_VMEM,
        scratch_shapes=[
            pltpu.VMEM((2, tokens, steps * 128), BF16),
            pltpu.VMEM(eig.shape, BF16),
            pltpu.SemaphoreType.DMA((2, steps)),
            pltpu.SemaphoreType.DMA,
        ],
        name="project",
    )(inputs, upstream, eig)


def spread_kernel(parts_ref, own_ref, copies_ref, halves_ref):
    total = parts_ref[0].astype(F32)
    for k in range(1, parts_ref.shape[0]):
        total += parts_ref[k].astype(F32)
    own = total.astype(BF16)
    own_ref[...] = own
    for k in range(copies_ref.shape[0]):
        copies_ref[k] = own
    for core in range(2):
        for k in range(8):
            halves_ref[core * 8 + k] = own[:, core * 32 : core * 32 + 32]


def gram_kernel(b_ref, a_ref, other_ref, out_ref):
    core = lax.axis_index("core")
    tokens = a_ref.shape[3]
    block = jnp.zeros(out_ref.shape, F32).reshape(256, -1)
    for of, ref in ((core, a_ref), (core ^ 1, other_ref)):
        for s in range(2):
            block += lax.dot_general(
                b_ref[of, :, s].reshape(256, tokens),
                ref[:, 1 - s].reshape(-1, tokens),
                (((1,), (1,)), ((), ())),
                preferred_element_type=F32,
            )
    out_ref[...] = block.astype(BF16).reshape(out_ref.shape)


def roots_kernel(*refs):
    for k in range(3):
        refs[3 + k][...] = jnp.sqrt(refs[k][...])


def weigh_kernel(parts_ref, rows_ref, cols_ref, out_ref):
    share = parts_ref[0].astype(F32)
    for k in range(1, parts_ref.shape[0]):
        share += parts_ref[k].astype(F32)
    s_b, s_a = rows_ref[...], cols_ref[...]
    kernel = -1.0 / (s_b * s_a * (s_b + s_a))
    part = (kernel * (0.5 * share)).astype(BF16)
    for k in range(out_ref.shape[0]):
        out_ref[k] = part


def mix_kernel(half_ref, a_ref, other_ref, out_ref):
    core = lax.axis_index("core")
    tokens = a_ref.shape[3]
    weights = half_ref[...].reshape(256, -1)
    for to, ref in ((core, a_ref), (core ^ 1, other_ref)):
        proj_in = ref[:, 0].reshape(-1, tokens)
        part = jnp.dot(weights, proj_in, preferred_element_type=F32)
        out_ref[to] = part.astype(BF16).reshape(8, 32, tokens)


def update_kernel(factor, parts_ref, own_ref, root_ref, out_ref):
    for half in range(2):
        mixed = parts_ref[half, 0].astype(F32)
        for k in range(1, 8):
            mixed += parts_ref[half, k].astype(F32)
        rows = pl.ds(half * 32, 32)
        update = own_ref[1, rows].astype(F32) / root_ref[rows] + factor * mixed
        update = update.astype(BF16)
        for k in range(out_ref.shape[0]):
            out_ref[k, rows] = update


def split_l_kernel(kept_ref, came_ref, keep_ref, send_ref):
    zl, xl = lax.axis_index("zl"), lax.axis_index("xl")
    for from_z, ref in ((zl, kept_ref), (zl ^ 1, came_ref)):
        for to_h in range(2):
            keep_ref[from_z, to_h] = ref[to_h * 2 + xl]
            send_ref[from_z, to_h] = ref[to_h * 2 + (xl ^ 1)]


def split_h_kernel(kept_ref, came_ref, keep_ref, send_ref):
    xh, xl = lax.axis_index("xh"), lax.axis_index("xl")
    for from_l, ref in ((xl, kept_ref), (xl ^ 1, came_ref)):
        for from_z in range(2):
            keep_ref[from_z, from_l] = ref[from_z, xh]
            send_ref[from_z, from_l] = ref[from_z, xh ^ 1]


def finish_kernel(kept_ref, came_ref, every_ref, out_ref, basis):
    xh = lax.axis_index("xh")
    tokens = every_ref.shape[2]
    for from_h, ref in ((xh, kept_ref), (xh ^ 1, came_ref)):
        for from_z in range(2):
            blocks = [ref[from_z, from_l, lb] for from_l in range(2) for lb in range(2)]
            basis[from_z * 2 + from_h] = jnp.concatenate(blocks, 1)
    part = jnp.dot(
        basis[...].reshape(512, 512),
        every_ref[...].reshape(512, tokens),
        preferred_element_type=F32,
    )
    part = part.astype(BF16).reshape(8, 64, tokens)
    for y in range(8):
        out_ref[(y & 1) * 4 + (y & 2) + (y >> 2)] = part[y]


def on_device(inputs, upstream, eig_tiles, eigvals):
    zl, xh, xl, core = (lax.axis_index(a) for a in ("zl", "xh", "xl", "core"))
    y = lax.axis_index(("y2", "y1", "y0"))
    share = lax.axis_index(DEPTH)
    tokens = inputs.shape[0]
    eig = eig_tiles[0]
    r = zl * 2 + xh

    by_b = lax.dynamic_index_in_dim(eigvals.reshape(2, 2, 8, 128), y, 2, keepdims=False)
    lam_b = jnp.transpose(by_b, (1, 0, 2)).reshape(8, 64)
    cube = jnp.transpose(eigvals.reshape(2, 2, 8, 2, 64), (0, 3, 1, 2, 4)).reshape(8, 8, 64)
    lam_a = lax.dynamic_index_in_dim(cube, r * 2 + xl, 0, keepdims=False)
    lam_own = lax.dynamic_index_in_dim(lam_a, y, 0, keepdims=False).reshape(64, 1)
    by_place = jnp.transpose(lam_b.reshape(2, 2, 2, 64), (2, 0, 1, 3)).reshape(4, 2, 2, 32)
    by_core = lax.dynamic_index_in_dim(by_place, core, 2, keepdims=False)
    lam_rows = lax.dynamic_index_in_dim(by_core, share, 0, keepdims=False).reshape(64, 1)
    lam_cols = jnp.transpose(lam_a.reshape(2, 2, 2, 64), (2, 1, 0, 3)).reshape(1, 512)

    parts = project(inputs, upstream, eig)
    got = lax.all_to_all(parts, ROWS, 0, 0, tiled=True)
    own, copies, pieces = call(
        spread_kernel,
        (got,),
        (
            out(BF16, 2, 64, tokens),
            out(BF16, 8, 2, 64, tokens),
            out(BF16, 16, 2, 32, tokens),
        ),
    )
    halves = eig.reshape(2, 4, 2, 128, 128)
    right = lax.all_to_all(copies, LINE, 0, 0, tiled=True)
    away = lax.dynamic_index_in_dim(halves, 1 - zl, 0, keepdims=False)
    kept = lax.dynamic_index_in_dim(halves, zl, 0, keepdims=False)
    came = lax.ppermute(away, "zl", SWAP)
    quarter = out(BF16, 2, 2, 2, 128, 128)
    keep_l, send_l = call(split_l_kernel, (kept, came), (quarter, quarter))
    got_l = lax.ppermute(send_l, "xl", SWAP)
    s_rows, s_cols, s_own = call(
        roots_kernel,
        (lam_rows, lam_cols, lam_own),
        (out(F32, 64, 1), out(F32, 1, 512), out(F32, 64, 1)),
    )
    left = lax.all_to_all(pieces, CHIPS, 0, 0, tiled=True)
    other = lax.ppermute(right, "core", SWAP)
    both = call(
        gram_kernel, (left.reshape(2, 8, 2, 32, tokens), right, other), out(BF16, 4, 64, 512)
    )

    shares = lax.all_to_all(both, DEPTH, 0, 0, tiled=True)
    keep_h, send_h = call(split_h_kernel, (keep_l, got_l), (quarter, quarter))
    got_h = lax.ppermute(send_h, "xh", SWAP)
    part = call(weigh_kernel, (shares, s_rows, s_cols), out(BF16, 4, 64, 512))
    mine = lax.all_to_all(part, DEPTH, 0, 0, tiled=True)
    mixed_part = call(mix_kernel, (mine, right, other), out(BF16, 2, 8, 32, tokens))
    mixed = lax.all_to_all(
        mixed_part.reshape(16, 32, tokens), CHIPS, 0, 0, tiled=True
    )
    factor = 2.0 / (8 * tokens)
    update = call(
        lambda *refs: update_kernel(factor, *refs),
        (mixed.reshape(2, 8, 32, tokens), own, s_own),
        out(BF16, 8, 64, tokens),
    )
    every = lax.all_to_all(update, COLS, 0, 0, tiled=True)
    grad_part = call(
        finish_kernel,
        (keep_h, got_h, every),
        out(BF16, 8, 64, tokens),
        (pltpu.VMEM((4, 128, 512), BF16),),
    )
    blocks = lax.all_to_all(grad_part, LINE, 0, 0, tiled=True)
    return jnp.sum(blocks.astype(F32), 0).astype(BF16)


def solution(mesh):
    grid = Mesh(mesh.devices.reshape(SIZES), AXES)
    dp, mp = AXES[:3], AXES[3:]
    return jax.shard_map(
        on_device,
        mesh=grid,
        in_specs=(P(dp, None), P(dp, None), P(mp, None, None, None, None), P()),
        out_specs=P(mp, dp),
        check_vma=False,
    )
```

```python
import jax
import jax.numpy as jnp
from jax import lax
from jax.experimental import pallas as pl
from jax.experimental.pallas import tpu as pltpu
from jax.sharding import Mesh
from jax.sharding import PartitionSpec as P

F32 = jnp.float32
BF16 = jnp.bfloat16
AXES = ("zh1", "zh0", "core", "zl", "xh", "xl", "y2", "y1", "y0")
SIZES = (2,) * 9
ROWS = ("xh", "zl")
LINE = ("y0", "y1", "y2")
DEPTH = ("zh0", "zh1")
COLS = ("xl", "zl", "xh")
CHIPS = ("core", "xh", "xl", "zl")
SWAP = [(0, 1), (1, 0)]

ANYWHERE = pl.BlockSpec(memory_space=pl.ANY)
IN_VMEM = pl.BlockSpec(memory_space=pltpu.VMEM)


def call(kernel, arrays, outs, scratch=()):
    held = [pltpu.with_memory_space_constraint(a, pltpu.VMEM) for a in arrays]
    single = not isinstance(outs, (list, tuple))
    shapes = [outs] if single else outs
    got = pl.pallas_call(
        kernel,
        out_shape=[pltpu.VMEM(s, d) for s, d in shapes_of(shapes)],
        in_specs=[IN_VMEM] * len(held),
        out_specs=[IN_VMEM] * len(shapes),
        scratch_shapes=list(scratch),
    )(*held)
    return got[0] if single else got


def shapes_of(outs):
    return [(o.shape, o.dtype) for o in outs]


def out(dtype, *shape):
    return jax.ShapeDtypeStruct(shape, dtype)


def project_kernel(x_ref, y_ref, eig_ref, out_ref, xs, tiles, sems, tile_sem):
    steps = eig_ref.shape[0]
    grid_rows = x_ref.shape[1] // (steps * 128)
    r = lax.axis_index("zl") * 2 + lax.axis_index("xh")

    def copy(s, la):
        src = x_ref if s == 0 else y_ref
        start = pl.multiple_of((la * grid_rows + r) * 128, 128)
        return pltpu.make_async_copy(
            src.at[:, pl.ds(start, 128)], xs.at[s, :, pl.ds(la * 128, 128)], sems.at[s, la]
        )

    load = pltpu.make_async_copy(eig_ref, tiles, tile_sem)
    load.start()
    for s in range(2):
        for la in range(steps):
            copy(s, la).start()
    load.wait()
    basis = jnp.concatenate(
        [tiles[:, lb].reshape(steps * 128, 128) for lb in range(tiles.shape[1])], 1
    )
    for s in range(2):
        for la in range(steps):
            copy(s, la).wait()
        part = jnp.dot(xs[s], basis, preferred_element_type=F32)
        turned = part.astype(BF16).T
        turned = turned.reshape(out_ref.shape[0], *out_ref.shape[2:])
        for zl in range(2):
            for xh in range(2):
                out_ref[xh * 2 + zl, s] = turned[zl * 2 + xh]


def project(inputs, upstream, eig):
    tokens = inputs.shape[0]
    steps = eig.shape[0]
    return pl.pallas_call(
        project_kernel,
        out_shape=pltpu.VMEM((4, 2, 64, tokens), BF16),
        in_specs=[ANYWHERE] * 3,
        out_specs=IN_VMEM,
        scratch_shapes=[
            pltpu.VMEM((2, tokens, steps * 128), BF16),
            pltpu.VMEM(eig.shape, BF16),
            pltpu.SemaphoreType.DMA((2, steps)),
            pltpu.SemaphoreType.DMA,
        ],
        name="project",
    )(inputs, upstream, eig)


def spread_kernel(parts_ref, own_ref, copies_ref):
    total = parts_ref[0].astype(F32)
    for k in range(1, parts_ref.shape[0]):
        total += parts_ref[k].astype(F32)
    own = total.astype(BF16)
    own_ref[...] = own
    for k in range(copies_ref.shape[0]):
        copies_ref[k] = own


def again_kernel(own_ref, out_ref):
    for core in range(2):
        for k in range(8):
            out_ref[core * 8 + k] = own_ref[:, core * 32 : core * 32 + 32]


def gram_kernel(b_ref, a_ref, other_ref, out_ref):
    core = lax.axis_index("core")
    tokens = a_ref.shape[3]
    block = jnp.zeros(out_ref.shape, F32).reshape(256, -1)
    for of, ref in ((core, a_ref), (core ^ 1, other_ref)):
        for s in range(2):
            block += lax.dot_general(
                b_ref[of, :, s].reshape(256, tokens),
                ref[:, 1 - s].reshape(-1, tokens),
                (((1,), (1,)), ((), ())),
                preferred_element_type=F32,
            )
    out_ref[...] = block.astype(BF16).reshape(out_ref.shape)


def roots_kernel(*refs):
    for k in range(3):
        refs[3 + k][...] = jnp.sqrt(refs[k][...])


def weigh_kernel(parts_ref, rows_ref, cols_ref, out_ref):
    share = parts_ref[0].astype(F32)
    for k in range(1, parts_ref.shape[0]):
        share += parts_ref[k].astype(F32)
    s_b, s_a = rows_ref[...], cols_ref[...]
    kernel = -1.0 / (s_b * s_a * (s_b + s_a))
    part = (kernel * (0.5 * share)).astype(BF16)
    for k in range(out_ref.shape[0]):
        out_ref[k] = part


def mix_kernel(half_ref, a_ref, other_ref, out_ref):
    core = lax.axis_index("core")
    tokens = a_ref.shape[3]
    weights = half_ref[...].reshape(256, -1)
    for to, ref in ((core, a_ref), (core ^ 1, other_ref)):
        proj_in = ref[:, 0].reshape(-1, tokens)
        part = jnp.dot(weights, proj_in, preferred_element_type=F32)
        out_ref[to] = part.astype(BF16).reshape(8, 32, tokens)


def update_kernel(factor, parts_ref, own_ref, root_ref, out_ref):
    for half in range(2):
        mixed = parts_ref[half, 0].astype(F32)
        for k in range(1, 8):
            mixed += parts_ref[half, k].astype(F32)
        rows = pl.ds(half * 32, 32)
        update = own_ref[1, rows].astype(F32) / root_ref[rows] + factor * mixed
        update = update.astype(BF16)
        for k in range(out_ref.shape[0]):
            out_ref[k, rows] = update


def split_l_kernel(kept_ref, came_ref, keep_ref, send_ref):
    zl, xl = lax.axis_index("zl"), lax.axis_index("xl")
    for from_z, ref in ((zl, kept_ref), (zl ^ 1, came_ref)):
        for to_h in range(2):
            keep_ref[from_z, to_h] = ref[to_h * 2 + xl]
            send_ref[from_z, to_h] = ref[to_h * 2 + (xl ^ 1)]


def split_h_kernel(kept_ref, came_ref, keep_ref, send_ref):
    xh, xl = lax.axis_index("xh"), lax.axis_index("xl")
    for from_l, ref in ((xl, kept_ref), (xl ^ 1, came_ref)):
        for from_z in range(2):
            keep_ref[from_z, from_l] = ref[from_z, xh]
            send_ref[from_z, from_l] = ref[from_z, xh ^ 1]


def finish_kernel(kept_ref, came_ref, every_ref, out_ref, basis):
    xh = lax.axis_index("xh")
    tokens = every_ref.shape[2]
    for from_h, ref in ((xh, kept_ref), (xh ^ 1, came_ref)):
        for from_z in range(2):
            blocks = [ref[from_z, from_l, lb] for from_l in range(2) for lb in range(2)]
            basis[from_z * 2 + from_h] = jnp.concatenate(blocks, 1)
    part = jnp.dot(
        basis[...].reshape(512, 512),
        every_ref[...].reshape(512, tokens),
        preferred_element_type=F32,
    )
    part = part.astype(BF16).reshape(8, 64, tokens)
    for y in range(8):
        out_ref[(y & 1) * 4 + (y & 2) + (y >> 2)] = part[y]


def on_device(inputs, upstream, eig_tiles, eigvals):
    zl, xh, xl, core = (lax.axis_index(a) for a in ("zl", "xh", "xl", "core"))
    y = lax.axis_index(("y2", "y1", "y0"))
    share = lax.axis_index(DEPTH)
    tokens = inputs.shape[0]
    eig = eig_tiles[0]
    r = zl * 2 + xh

    by_b = lax.dynamic_index_in_dim(eigvals.reshape(2, 2, 8, 128), y, 2, keepdims=False)
    lam_b = jnp.transpose(by_b, (1, 0, 2)).reshape(8, 64)
    cube = jnp.transpose(eigvals.reshape(2, 2, 8, 2, 64), (0, 3, 1, 2, 4)).reshape(8, 8, 64)
    lam_a = lax.dynamic_index_in_dim(cube, r * 2 + xl, 0, keepdims=False)
    lam_own = lax.dynamic_index_in_dim(lam_a, y, 0, keepdims=False).reshape(64, 1)
    by_place = jnp.transpose(lam_b.reshape(2, 2, 2, 64), (2, 0, 1, 3)).reshape(4, 2, 2, 32)
    by_core = lax.dynamic_index_in_dim(by_place, core, 2, keepdims=False)
    lam_rows = lax.dynamic_index_in_dim(by_core, share, 0, keepdims=False).reshape(64, 1)
    lam_cols = jnp.transpose(lam_a.reshape(2, 2, 2, 64), (2, 1, 0, 3)).reshape(1, 512)

    parts = project(inputs, upstream, eig)
    got = lax.all_to_all(parts, ROWS, 0, 0, tiled=True)
    own, copies = call(
        spread_kernel, (got,), (out(BF16, 2, 64, tokens), out(BF16, 8, 2, 64, tokens))
    )
    halves = eig.reshape(2, 4, 2, 128, 128)
    right = lax.all_to_all(copies, LINE, 0, 0, tiled=True)
    away = lax.dynamic_index_in_dim(halves, 1 - zl, 0, keepdims=False)
    kept = lax.dynamic_index_in_dim(halves, zl, 0, keepdims=False)
    came = lax.ppermute(away, "zl", SWAP)
    quarter = out(BF16, 2, 2, 2, 128, 128)
    keep_l, send_l = call(split_l_kernel, (kept, came), (quarter, quarter))
    got_l = lax.ppermute(send_l, "xl", SWAP)
    s_rows, s_cols, s_own = call(
        roots_kernel,
        (lam_rows, lam_cols, lam_own),
        (out(F32, 64, 1), out(F32, 1, 512), out(F32, 64, 1)),
    )
    again = call(again_kernel, (own,), out(BF16, 16, 2, 32, tokens))
    left = lax.all_to_all(again, CHIPS, 0, 0, tiled=True)
    other = lax.ppermute(right, "core", SWAP)
    both = call(
        gram_kernel, (left.reshape(2, 8, 2, 32, tokens), right, other), out(BF16, 4, 64, 512)
    )

    shares = lax.all_to_all(both, DEPTH, 0, 0, tiled=True)
    keep_h, send_h = call(split_h_kernel, (keep_l, got_l), (quarter, quarter))
    got_h = lax.ppermute(send_h, "xh", SWAP)
    part = call(weigh_kernel, (shares, s_rows, s_cols), out(BF16, 4, 64, 512))
    mine = lax.all_to_all(part, DEPTH, 0, 0, tiled=True)
    mixed_part = call(mix_kernel, (mine, right, other), out(BF16, 2, 8, 32, tokens))
    mixed = lax.all_to_all(
        mixed_part.reshape(16, 32, tokens), CHIPS, 0, 0, tiled=True
    )
    factor = 2.0 / (8 * tokens)
    update = call(
        lambda *refs: update_kernel(factor, *refs),
        (mixed.reshape(2, 8, 32, tokens), own, s_own),
        out(BF16, 8, 64, tokens),
    )
    every = lax.all_to_all(update, COLS, 0, 0, tiled=True)
    grad_part = call(
        finish_kernel,
        (keep_h, got_h, every),
        out(BF16, 8, 64, tokens),
        (pltpu.VMEM((4, 128, 512), BF16),),
    )
    blocks = lax.all_to_all(grad_part, LINE, 0, 0, tiled=True)
    return jnp.sum(blocks.astype(F32), 0).astype(BF16)


def solution(mesh):
    grid = Mesh(mesh.devices.reshape(SIZES), AXES)
    dp, mp = AXES[:3], AXES[3:]
    return jax.shard_map(
        on_device,
        mesh=grid,
        in_specs=(P(dp, None), P(dp, None), P(mp, None, None, None, None), P()),
        out_specs=P(mp, dp),
        check_vma=False,
    )
```
